32 devices in a mesh: band: 8 (over z, y), dir: 4 (over x, core).
Axes of the slice: x: 2, y: 2, z: 4, core: 2. Of those that a mesh axis runs over, the one named last changes fastest.
Arguments:
- visibilities: float32 [8, 2, 2, 2, 16, 512], P('band'), may hold values from -6 to 6
- coherencies: float32 [8, 16, 2, 2, 2, 16, 512], P('band', 'dir'), may hold values from -1.2 to 1.2
- jones_start: float32 [8, 16, 2, 2, 2, 1024], P('band', 'dir'), may hold values from -3.6 to 3.6
- dual_start: float32 [8, 16, 2, 2, 2, 1024], P('band', 'dir'), may hold values from -6 to 6
- consensus_start: float32 [8, 16, 2, 2, 2, 1024], P(None, 'dir'), may hold values from -1.8 to 1.8
- freq_basis: float32 [8, 8], P('band'), may hold values from -1 to 1
- baseline_station_pairs: int32 [2, 512], replicated, may hold values from 0 to 1023
Outputs:
- jones_final: float32 [8, 16, 2, 2, 2, 1024], P('band', 'dir')
- dual_final: float32 [8, 16, 2, 2, 2, 1024], P('band', 'dir')
- consensus_coeffs: float32 [8, 16, 2, 2, 2, 1024], P(None, 'dir')
The draws below stay inside these ranges and needn't reach their ends.
All inputs are finite; a program needn't handle non-finite values.
Results may differ from the reference program's by a relative error of at most 0.0003.
Values sent between devices are 32-bit elements; how exact they have to be, the bound alone decides.
No kernel may reach another device: no remote copies, remote signals or barrier semaphores. Data moves between devices by JAX's collectives and lax.ppermute only.
A program may use at most 128 MiB of HBM per device.

```python
import jax
import jax.numpy as jnp
from jax import lax

STATION_COUNT = 1024
TERMS = 8
TIMESLOT_COUNT = 16
BASELINE_COUNT = 512
ITERS = 3
DIRECTION_COUNT = 16
SUBBAND_COUNT = 8


def place_ends(drawn, own_key, least, top_value):
    spot = [jax.random.randint(jax.random.fold_in(own_key, axis), (), 0, length) for axis, length in enumerate(drawn.shape)]
    widest = drawn.shape.index(max(drawn.shape))
    neighbour = spot[:widest] + [(spot[widest] + 1) % drawn.shape[widest]] + spot[widest + 1:]
    return drawn.at[tuple(spot)].set(least).at[tuple(neighbour)].set(top_value)


def block_levels(key, shape, cuts, low, high):
    loudness = 1.0
    for position, shards_of in cuts:
        draws = jax.random.uniform(jax.random.fold_in(jax.random.fold_in(key, 6), position), (shards_of,), jnp.float32, low / len(cuts), high / len(cuts))
        loudness = loudness * jnp.repeat(jnp.exp(draws), shape[position] // shards_of).reshape((-1,) + (1,) * (len(shape) - 1 - position))
    return loudness


def normal_values(own_key, shape, scale, bound, pieces=(), held_as=jnp.bfloat16):
    loudness = block_levels(own_key, shape, pieces, -0.22, 0.18) if pieces else 1.0
    array = jax.random.normal(own_key, shape, jnp.float32) * scale * loudness
    return jnp.minimum(jnp.maximum(array, -bound), bound).astype(held_as)


def setup_inputs(seed: int = 0) -> dict:
    key_of = jax.random.split(jax.random.key(seed), 8)
    visibilities = normal_values(key_of[0], (SUBBAND_COUNT, 2, 2, 2, TIMESLOT_COUNT, BASELINE_COUNT), 1.0, 6.0, ((0, 8),), jnp.float32)
    coherencies = normal_values(key_of[1], (SUBBAND_COUNT, DIRECTION_COUNT, 2, 2, 2, TIMESLOT_COUNT, BASELINE_COUNT), 0.2, 1.2, ((0, 8), (1, 4)), jnp.float32)
    jones_start = normal_values(key_of[2], (SUBBAND_COUNT, DIRECTION_COUNT, 2, 2, 2, STATION_COUNT), 0.6, 3.6, ((0, 8), (1, 4)), jnp.float32)
    dual_start = normal_values(key_of[3], (SUBBAND_COUNT, DIRECTION_COUNT, 2, 2, 2, STATION_COUNT), 1.0, 6.0, ((0, 8), (1, 4)), jnp.float32)
    consensus_start = normal_values(key_of[4], (TERMS, DIRECTION_COUNT, 2, 2, 2, STATION_COUNT), 0.3, 1.8, ((1, 4),), jnp.float32)
    freq_basis = jnp.clip(jax.random.uniform(key_of[5], (SUBBAND_COUNT, TERMS), jnp.float32, -1.0, 1.0) * block_levels(key_of[5], (SUBBAND_COUNT, TERMS), ((0, 8),), -0.4, 0.0), -1.0, 1.0)
    baseline_station_pairs = place_ends(jax.random.randint(key_of[6], (2, BASELINE_COUNT), 0, STATION_COUNT), jax.random.fold_in(key_of[6], 1), 0, STATION_COUNT - 1).astype(jnp.int32)
    return dict(visibilities=visibilities, coherencies=coherencies, jones_start=jones_start, dual_start=dual_start, consensus_start=consensus_start, freq_basis=freq_basis, baseline_station_pairs=baseline_station_pairs)


RHO = 5.0
RIDGE = 0.25

def small_mul(left, right):
    return left[:, 0:1] * right[0:1] + left[:, 1:2] * right[1:2]

def complex_mul(left, right):
    real_part = small_mul(left[0], right[0]) - small_mul(left[1], right[1])
    imag_part = small_mul(left[0], right[1]) + small_mul(left[1], right[0])
    return jnp.stack([real_part, imag_part])

def hermitian(value):
    return jnp.stack([jnp.swapaxes(value[0], 0, 1), -jnp.swapaxes(value[1], 0, 1)])

def solve_right(numer, matrix):
    adjugate = jnp.stack([jnp.stack([matrix[:, 1, 1], -matrix[:, 0, 1]], axis=1), jnp.stack([-matrix[:, 1, 0], matrix[:, 0, 0]], axis=1)], axis=1)
    det_real = matrix[0, 0, 0] * matrix[0, 1, 1] - matrix[1, 0, 0] * matrix[1, 1, 1] - (matrix[0, 0, 1] * matrix[0, 1, 0] - matrix[1, 0, 1] * matrix[1, 1, 0])
    det_imag = matrix[0, 0, 0] * matrix[1, 1, 1] + matrix[1, 0, 0] * matrix[0, 1, 1] - (matrix[0, 0, 1] * matrix[1, 1, 0] + matrix[1, 0, 1] * matrix[0, 1, 0])
    product = complex_mul(numer, adjugate)
    divisor = det_real * det_real + det_imag * det_imag
    real_part = (product[0] * det_real + product[1] * det_imag) / divisor
    imag_part = (product[1] * det_real - product[0] * det_imag) / divisor
    return jnp.stack([real_part, imag_part])

def predict(jones_k, coher_k, first, second):
    jones_first = jnp.take(jones_k, first, axis=-1)[..., None, :]
    jones_second = jnp.take(jones_k, second, axis=-1)[..., None, :]
    return complex_mul(complex_mul(jones_first, coher_k), hermitian(jones_second))

def baseline_terms(target, jones_k, coher_k, first, second):
    jones_first = jnp.take(jones_k, first, axis=-1)[..., None, :]
    jones_second = jnp.take(jones_k, second, axis=-1)[..., None, :]
    along_term = complex_mul(coher_k, hermitian(jones_second))
    back_term = hermitian(complex_mul(jones_first, coher_k))
    flipped = hermitian(target)
    right_first = jnp.sum(complex_mul(target, hermitian(along_term)), axis=-2)
    normal_first = jnp.sum(complex_mul(along_term, hermitian(along_term)), axis=-2)
    right_second = jnp.sum(complex_mul(flipped, hermitian(back_term)), axis=-2)
    normal_second = jnp.sum(complex_mul(back_term, hermitian(back_term)), axis=-2)
    first_part = jnp.concatenate([right_first.reshape(8, -1), normal_first.reshape(8, -1)], axis=0)
    second_part = jnp.concatenate([right_second.reshape(8, -1), normal_second.reshape(8, -1)], axis=0)
    return jnp.concatenate([first_part, second_part], axis=1)

def update_one(right_sum, normal_sum, consensus, dual):
    identity = jnp.stack([jnp.eye(2, dtype=jnp.float32), jnp.zeros((2, 2), jnp.float32)])[..., None]
    matrix = normal_sum + RHO * identity
    return solve_right(right_sum + RHO * consensus - dual, matrix)

def update_band(band_items, first, second):
    vis, coher, jones, dual, consensus = band_items
    stations = jones.shape[-1]
    dirs = jones.shape[0]
    model_terms = jax.vmap(predict, (0, 0, None, None))(jones, coher, first, second)
    residual = vis - jnp.sum(model_terms, axis=0)
    normal_terms = jax.vmap(baseline_terms, (0, 0, 0, None, None))(residual[None] + model_terms, jones, coher, first, second)
    stacked = normal_terms.reshape(dirs * 16, -1)
    segment_ids = jnp.concatenate([first, second]).astype(jnp.int32)
    segment = jax.ops.segment_sum(stacked.T, segment_ids, num_segments=stations).T
    segment = segment.reshape((dirs, 2, 2, 2, 2, stations))
    return jax.vmap(update_one)(segment[:, 0], segment[:, 1], consensus, dual)

def reference(visibilities, coherencies, jones_start, dual_start, consensus_start, freq_basis, baseline_station_pairs):
    first = baseline_station_pairs[0]
    second = baseline_station_pairs[1]
    terms = freq_basis.shape[1]
    gram = jnp.dot(freq_basis.T, freq_basis, precision=lax.Precision.HIGHEST) + RIDGE * freq_basis.shape[0] * jnp.eye(terms, dtype=jnp.float32)
    scale_factor = jnp.linalg.cholesky(gram)
    jones = jones_start
    dual = dual_start
    coeffs = consensus_start
    consensus = jnp.einsum('fm,mkabcs->fkabcs', freq_basis, coeffs, precision=lax.Precision.HIGHEST)
    for turn_index in range(ITERS):
        jones = lax.map(lambda band_items: update_band(band_items, first, second), (visibilities, coherencies, jones, dual, consensus))
        coeff_sums = jnp.einsum('fm,fkabcs->mkabcs', freq_basis, jones + dual / RHO, precision=lax.Precision.HIGHEST)
        flat = coeff_sums.reshape(terms, -1)
        coeffs = jax.scipy.linalg.cho_solve((scale_factor, True), flat).reshape(coeff_sums.shape)
        consensus = jnp.einsum('fm,mkabcs->fkabcs', freq_basis, coeffs, precision=lax.Precision.HIGHEST)
        dual = dual + RHO * (jones - consensus)
    return (jones, dual, coeffs)
```

```python
import functools

import jax
import jax.numpy as jnp
from jax import lax
from jax.experimental import pallas as pl
from jax.experimental.pallas import tpu as pltpu
from jax.sharding import PartitionSpec as P

ITERS = 3
RHO = 5.0
RIDGE = 0.25
LANES = 128
SUBLANES = 8

VMEM = pl.BlockSpec(memory_space=pltpu.VMEM)
SMEM = pl.BlockSpec(memory_space=pltpu.SMEM)
PARAMS = pltpu.CompilerParams(vmem_limit_bytes=48 * 1024 * 1024)

INDEX = ((0, 0), (0, 1), (1, 0), (1, 1))


def comp(part, i, j):
    return part * 4 + i * 2 + j


def cadd(a, b):
    return (a[0] + b[0], a[1] + b[1])


def cmul(a, b):
    return (a[0] * b[0] - a[1] * b[1], a[0] * b[1] + a[1] * b[0])


def cmul_conj(a, b):
    return (a[0] * b[0] + a[1] * b[1], a[1] * b[0] - a[0] * b[1])


def mat_mul(a, b):
    return {(i, j): cadd(cmul(a[i, 0], b[0, j]), cmul(a[i, 1], b[1, j])) for i, j in INDEX}


def mat_mul_h(a, b):
    return {(i, j): cadd(cmul_conj(a[i, 0], b[j, 0]), cmul_conj(a[i, 1], b[j, 1])) for i, j in INDEX}


def mat_h_mul(a, b):
    return {(i, j): cadd(cmul_conj(b[0, j], a[0, i]), cmul_conj(b[1, j], a[1, i])) for i, j in INDEX}


def sq(a):
    return a[0] * a[0] + a[1] * a[1]


def split_dot(left, right, dims):
    high = left.astype(jnp.bfloat16)
    low = (left - high.astype(jnp.float32)).astype(jnp.bfloat16)
    both = jnp.concatenate([high, low], axis=0)
    out = lax.dot_general(both, right, (dims, ((), ())), preferred_element_type=jnp.float32)
    return out[: left.shape[0]] + out[left.shape[0] :]


def onehot_kernel(pairs_ref, out_ref):
    stations = out_ref.shape[0]
    baselines = pairs_ref.shape[1]
    for half in range(2):
        ids = pairs_ref[half : half + 1, :]
        for base in range(0, stations, LANES):
            station = lax.broadcasted_iota(jnp.int32, (LANES, baselines), 0) + base
            hit = jnp.where(station == ids, 1.0, 0.0).astype(jnp.bfloat16)
            out_ref[base : base + LANES, half * baselines : (half + 1) * baselines] = hit


def read_rows(ref, dirs, k, base, width):
    def one(part, i, j):
        row = comp(part, i, j) * dirs + k
        return jnp.broadcast_to(ref[row : row + 1, base : base + width], (SUBLANES, width))

    return {(i, j): (one(0, i, j), one(1, i, j)) for i, j in INDEX}


def model_kernel(parity_ref, jones_ref, onehot_ref, coher_ref, gathered_ref, mine_ref, other_ref):
    dirs = coher_ref.shape[0]
    times, baselines = coher_ref.shape[-2:]
    gathered_ref[...] = split_dot(jones_ref[...], onehot_ref[...], ((1,), (0,)))
    first = parity_ref[0, 0] == 0
    for base in range(0, baselines, LANES):
        lanes = slice(base, base + LANES)
        for time in range(0, times, SUBLANES):
            rows = slice(time, time + SUBLANES)
            total = None
            for k in range(dirs):
                jones_p = read_rows(gathered_ref, dirs, k, base, LANES)
                jones_q = read_rows(gathered_ref, dirs, k, baselines + base, LANES)
                coher = {(i, j): tuple(coher_ref[k, part, i, j, rows, lanes] for part in range(2)) for i, j in INDEX}
                model = mat_mul(jones_p, mat_mul_h(coher, jones_q))
                total = model if total is None else {ij: cadd(total[ij], model[ij]) for ij in INDEX}
            for i, j in INDEX:
                real, imag = total[i, j]
                mine_ref[i, j, rows, lanes] = jnp.where(first, real, imag)
                other_ref[i, j, rows, lanes] = jnp.where(first, imag, real)


def solve_body(parity_ref, gathered_ref, onehot_ref, coher_ref, vis_ref, mine_ref, other_ref, left_ref, numer):
    dirs = coher_ref.shape[0]
    times, baselines = coher_ref.shape[-2:]
    first = parity_ref[0, 0] == 0
    for base in range(0, baselines, LANES):
        lanes = slice(base, base + LANES)
        resid = []
        for time in range(0, times, SUBLANES):
            rows = slice(time, time + SUBLANES)
            piece = {}
            for i, j in INDEX:
                mine = mine_ref[i, j, rows, lanes]
                other = other_ref[i, j, rows, lanes]
                piece[i, j] = (
                    vis_ref[0, i, j, rows, lanes] - jnp.where(first, mine, other),
                    vis_ref[1, i, j, rows, lanes] - jnp.where(first, other, mine),
                )
            resid.append(piece)
        for k in range(dirs):
            jones_p = read_rows(gathered_ref, dirs, k, base, LANES)
            jones_q = read_rows(gathered_ref, dirs, k, baselines + base, LANES)
            sums = None
            for index, time in enumerate(range(0, times, SUBLANES)):
                rows = slice(time, time + SUBLANES)
                coher = {(i, j): tuple(coher_ref[k, part, i, j, rows, lanes] for part in range(2)) for i, j in INDEX}
                along = mat_mul_h(coher, jones_q)
                ahead = mat_mul(jones_p, coher)
                right_p = mat_mul_h(resid[index], along)
                right_q = mat_h_mul(resid[index], ahead)
                cross_p = cadd(cmul_conj(along[0, 0], along[1, 0]), cmul_conj(along[0, 1], along[1, 1]))
                cross_q = cadd(cmul_conj(ahead[0, 1], ahead[0, 0]), cmul_conj(ahead[1, 1], ahead[1, 0]))
                terms_p = [right_p[ij][part] for part in range(2) for ij in INDEX] + [
                    sq(along[0, 0]) + sq(along[0, 1]),
                    sq(along[1, 0]) + sq(along[1, 1]),
                    cross_p[0],
                    cross_p[1],
                ]
                terms_q = [right_q[ij][part] for part in range(2) for ij in INDEX] + [
                    sq(ahead[0, 0]) + sq(ahead[1, 0]),
                    sq(ahead[0, 1]) + sq(ahead[1, 1]),
                    cross_q[0],
                    cross_q[1],
                ]
                terms = terms_p + terms_q
                sums = terms if sums is None else [a + b for a, b in zip(sums, terms)]
            for at, term in enumerate(sums):
                row = (at % 12) * dirs + k
                offset = base + (at // 12) * baselines
                left_ref[row : row + 1, offset : offset + LANES] = jnp.sum(term, axis=0, keepdims=True)

    def group(ref, at):
        return ref[at * dirs : (at + 1) * dirs, :]

    jones = {(i, j): (group(gathered_ref, comp(0, i, j)), group(gathered_ref, comp(1, i, j))) for i, j in INDEX}
    diag0, diag1 = group(left_ref, 8), group(left_ref, 9)
    off = (group(left_ref, 10), group(left_ref, 11))
    off_c = (off[0], -off[1])
    for i in range(2):
        left, right = jones[i, 0], jones[i, 1]
        col0 = cadd((left[0] * diag0, left[1] * diag0), cmul(right, off_c))
        col1 = cadd(cmul(left, off), (right[0] * diag1, right[1] * diag1))
        for j, col in ((0, col0), (1, col1)):
            for part in range(2):
                at = comp(part, i, j) * dirs
                left_ref[at : at + dirs, :] = left_ref[at : at + dirs, :] + col[part]

    sums = split_dot(left_ref[...], onehot_ref[...], ((1,), (1,)))
    m00 = sums[8 * dirs : 9 * dirs] + RHO
    m11 = sums[9 * dirs : 10 * dirs] + RHO
    m01 = (sums[10 * dirs : 11 * dirs], sums[11 * dirs : 12 * dirs])
    m10 = (m01[0], -m01[1])
    scale = 1.0 / (m00 * m11 - sq(m01))
    out = {}
    for i in range(2):
        n = []
        for j in range(2):
            at = [comp(part, i, j) * dirs for part in range(2)]
            n.append(tuple(sums[a : a + dirs] + numer(a) for a in at))
        x0 = cmul(n[1], m10)
        x1 = cmul(n[0], m01)
        out[i, 0] = tuple((n[0][part] * m11 - x0[part]) * scale for part in range(2))
        out[i, 1] = tuple((n[1][part] * m00 - x1[part]) * scale for part in range(2))
    return out


def first_solve_kernel(
    parity_ref, gathered_ref, onehot_ref, coher_ref, vis_ref, mine_ref, other_ref, consensus_ref, dual_ref,
    jones_ref, shared_ref, left_ref,
):
    dirs = coher_ref.shape[0]

    def numer(a):
        return RHO * consensus_ref[a : a + dirs, :] - dual_ref[a : a + dirs, :]

    out = solve_body(
        parity_ref, gathered_ref, onehot_ref, coher_ref, vis_ref, mine_ref, other_ref, left_ref, numer
    )
    write_solved(out, dirs, jones_ref, shared_ref, lambda a: dual_ref[a : a + dirs, :])


def write_solved(out, dirs, jones_ref, shared_ref, dual):
    for (i, j), parts in out.items():
        for part in range(2):
            a = comp(part, i, j) * dirs
            jones_ref[a : a + dirs, :] = parts[part]
            value = parts[part] + dual(a) * (1.0 / RHO)
            if len(shared_ref.shape) == 2:
                shared_ref[a : a + dirs, :] = value
            else:
                width = shared_ref.shape[2]
                for chunk in range(shared_ref.shape[0]):
                    shared_ref[chunk, a : a + dirs, :] = value[:, chunk * width : (chunk + 1) * width]


def next_solve_kernel(
    parity_ref, gathered_ref, onehot_ref, coher_ref, vis_ref, mine_ref, other_ref, consensus_ref, dual_ref, before_ref,
    jones_ref, shared_ref, dual_out_ref, left_ref,
):
    dirs = coher_ref.shape[0]

    def consensus(a):
        if len(consensus_ref.shape) == 2:
            return consensus_ref[a : a + dirs, :]
        pieces = [consensus_ref[chunk, a : a + dirs, :] for chunk in range(consensus_ref.shape[0])]
        return jnp.concatenate(pieces, axis=1)

    for a in range(0, 8 * dirs, dirs):
        dual_out_ref[a : a + dirs, :] = dual_ref[a : a + dirs, :] + RHO * (before_ref[a : a + dirs, :] - consensus(a))

    def numer(a):
        return RHO * consensus(a) - dual_out_ref[a : a + dirs, :]

    out = solve_body(
        parity_ref, gathered_ref, onehot_ref, coher_ref, vis_ref, mine_ref, other_ref, left_ref, numer
    )
    write_solved(out, dirs, jones_ref, shared_ref, lambda a: dual_out_ref[a : a + dirs, :])


def weights_kernel(basis_ref, weights_ref):
    bands, terms = basis_ref.shape
    basis = basis_ref[...]
    hi = lax.Precision.HIGHEST
    gram = lax.dot_general(basis, basis, (((0,), (0,)), ((), ())), precision=hi, preferred_element_type=jnp.float32)
    row = lax.broadcasted_iota(jnp.int32, (terms, terms), 0)
    col = lax.broadcasted_iota(jnp.int32, (terms, terms), 1)
    gram = gram + jnp.where(row == col, RIDGE * bands, 0.0)
    inverse = jnp.where(row == col, 1.0, 0.0)
    for t in range(terms):
        scale = 1.0 / gram[t : t + 1, t : t + 1]
        g_row = gram[t : t + 1, :] * scale
        i_row = inverse[t : t + 1, :] * scale
        factor = gram[:, t : t + 1]
        here = row == t
        gram = jnp.where(here, g_row, gram - factor * g_row)
        inverse = jnp.where(here, i_row, inverse - factor * i_row)
    weights = lax.dot_general(inverse, basis, (((1,), (1,)), ((), ())), precision=hi, preferred_element_type=jnp.float32)
    weights_ref[:terms, :] = weights
    weights_ref[terms:, :] = jnp.dot(basis, weights, precision=hi, preferred_element_type=jnp.float32)


def mix_kernel(weights_ref, shared_ref, out_ref):
    bands = shared_ref.shape[0]
    terms = weights_ref.shape[0] - bands
    values = [shared_ref[f] for f in range(bands)]
    for g in range(bands):
        total = values[0] * weights_ref[terms + g, 0]
        for f in range(1, bands):
            total = total + values[f] * weights_ref[terms + g, f]
        out_ref[g] = total


def final_kernel(weights_ref, own_ref, jones_ref, dual_ref, *refs):
    shared_refs, (coeffs_ref, dual_out_ref) = refs[:-2], refs[-2:]
    terms = weights_ref.shape[0]
    rows = jones_ref.shape[0]
    for r in range(0, rows, SUBLANES):
        span = slice(r, r + SUBLANES)
        values = [ref[span, :] for ref in shared_refs]
        consensus = None
        for m in range(terms):
            total = values[0] * weights_ref[m, 0]
            for f in range(1, len(values)):
                total = total + values[f] * weights_ref[m, f]
            coeffs_ref[m, span, :] = total
            part = total * own_ref[0, m]
            consensus = part if consensus is None else consensus + part
        dual_out_ref[span, :] = dual_ref[span, :] + RHO * (jones_ref[span, :] - consensus)


def struct(*shape, dtype=jnp.float32):
    return jax.ShapeDtypeStruct(shape, dtype)


def call(kernel, out_shape, in_specs, args, scratch=()):
    many = isinstance(out_shape, (tuple, list))
    return pl.pallas_call(
        kernel,
        out_shape=out_shape,
        in_specs=in_specs,
        out_specs=tuple(VMEM for _ in out_shape) if many else VMEM,
        scratch_shapes=list(scratch),
        compiler_params=PARAMS,
    )(*args)


def swap(value, axis, bit):
    size = lax.axis_size(axis)
    return lax.ppermute(value, axis, [(i, i ^ bit) for i in range(size)])


def to_rows(value):
    dirs, stations = value.shape[0], value.shape[-1]
    return value.reshape(dirs, 8, stations).transpose(1, 0, 2).reshape(8 * dirs, stations)


def from_rows(value, dirs):
    stations = value.shape[-1]
    lead = value.shape[:-2]
    value = value.reshape(lead + (8, dirs, stations))
    value = jnp.swapaxes(value, -3, -2)
    return value.reshape(lead + (dirs, 2, 2, 2, stations))


def sum_over_dir(mine, other):
    size = lax.axis_size("dir")
    mine = mine + swap(other, "dir", 1)
    bit = 2
    while bit < size:
        mine = mine + swap(mine, "dir", bit)
        bit *= 2
    return mine, swap(mine, "dir", 1)


def ring_gather(value):
    size = lax.axis_size("band")
    order = list(range(0, size, 2)) + list(range(size - 1, 0, -2))
    ahead = [(order[i], order[(i + 1) % size]) for i in range(size)]
    behind = [(b, a) for a, b in ahead]
    place = [order.index(i) for i in range(size)]
    at = jnp.asarray(place)[lax.axis_index("band")]
    order = jnp.asarray(order)
    values, sources = [value], [at]
    up = down = value
    for step in range(1, (size - 1) // 2 + 1):
        up = lax.ppermute(up, "band", ahead)
        down = lax.ppermute(down, "band", behind)
        values += [up, down]
        sources += [at - step, at + step]
    half = value.shape[0] // 2
    top = lax.ppermute(up[:half], "band", ahead)
    bottom = lax.ppermute(down[half:], "band", behind)
    values.append(jnp.concatenate([top, bottom], axis=0))
    sources.append(at + size // 2)
    return values, order[jnp.stack(sources) % size]


def local(visibilities, coherencies, jones_start, dual_start, consensus_start, freq_basis, pairs):
    row = freq_basis[0]
    terms = row.shape[0]
    bands = lax.axis_size("band")
    vis, coher = visibilities[0], coherencies[0]
    dirs, stations = jones_start.shape[1], jones_start.shape[-1]
    times, baselines = coher.shape[-2:]
    rows = 8 * dirs
    parity = (lax.axis_index("dir") % 2).astype(jnp.int32).reshape(1, 1)
    chunked = stations % (bands * LANES) == 0
    hi = lax.Precision.HIGHEST

    onehot = call(onehot_kernel, struct(stations, 2 * baselines, dtype=jnp.bfloat16), [VMEM], (pairs,))
    jones = to_rows(jones_start[0])
    dual = to_rows(dual_start[0])
    consensus = to_rows(jnp.tensordot(row, consensus_start, axes=(0, 0), precision=hi))
    half = struct(2, 2, times, baselines)
    flat = struct(rows, stations)
    left = pltpu.VMEM((12 * dirs, 2 * baselines), jnp.float32)

    if chunked:
        basis = lax.all_to_all(jnp.broadcast_to(freq_basis, (bands, terms)), "band", 0, 0, tiled=True)
        weights = call(weights_kernel, struct(terms + bands, bands), [VMEM], (basis,))
    else:
        gram = lax.psum(row[:, None] * row[None, :], "band") + RIDGE * bands * jnp.eye(terms, dtype=jnp.float32)
        factor = jnp.linalg.cholesky(gram)

    before = None
    for turn in range(ITERS):
        last = turn == ITERS - 1
        gathered, mine, other = call(
            model_kernel, (struct(rows, 2 * baselines), half, half), [SMEM, VMEM, VMEM, VMEM],
            (parity, jones, onehot, coher),
        )
        mine, other = sum_over_dir(mine, other)
        common = (parity, gathered, onehot, coher, vis, mine, other, consensus, dual)
        shared_shape = struct(bands, rows, stations // bands) if chunked and not last else flat
        if turn == 0:
            jones, shared = call(first_solve_kernel, (flat, shared_shape), [SMEM] + [VMEM] * 8, common, [left])
        else:
            jones, shared, dual = call(
                next_solve_kernel, (flat, shared_shape, flat), [SMEM] + [VMEM] * 9, common + (jones,), [left]
            )
        if last:
            break
        if chunked:
            shared = lax.all_to_all(shared, "band", 0, 0)
            mixed = call(mix_kernel, struct(*shared.shape), [SMEM, VMEM], (weights, shared))
            consensus = lax.all_to_all(mixed, "band", 0, 0)
        else:
            coeffs = reduce_bands(shared, row, factor)
            consensus = jnp.tensordot(row, coeffs, axes=(0, 0), precision=hi)
    if chunked:
        values, sources = ring_gather(shared)
        coeffs, dual = call(
            final_kernel, (struct(terms, rows, stations), flat), [SMEM, SMEM] + [VMEM] * (2 + len(values)),
            (weights[:terms][:, sources], freq_basis, jones, dual) + tuple(values),
        )
    else:
        coeffs = reduce_bands(shared, row, factor)
        dual = dual + RHO * (jones - jnp.tensordot(row, coeffs, axes=(0, 0), precision=hi))
    return from_rows(jones, dirs)[None], from_rows(dual, dirs)[None], from_rows(coeffs, dirs)


def reduce_bands(shared, row, factor):
    sums = lax.psum(row[:, None, None] * shared[None], "band")
    flat = sums.reshape(sums.shape[0], -1)
    return jax.scipy.linalg.cho_solve((factor, True), flat).reshape(sums.shape)


def solution(mesh):
    in_specs = (
        P("band", None, None, None, None, None),
        P("band", "dir", None, None, None, None, None),
        P("band", "dir", None, None, None, None),
        P("band", "dir", None, None, None, None),
        P(None, "dir", None, None, None, None),
        P("band", None),
        P(),
    )
    out_specs = (
        P("band", "dir", None, None, None, None),
        P("band", "dir", None, None, None, None),
        P(None, "dir", None, None, None, None),
    )
    return jax.shard_map(local, mesh=mesh, in_specs=in_specs, out_specs=out_specs, check_vma=False)
```

```python
import jax
import jax.numpy as jnp
from jax import lax
from jax.experimental import pallas as pl
from jax.experimental.pallas import tpu as pltpu
from jax.sharding import PartitionSpec as P

ITERS = 3
RHO = 5.0
RIDGE = 0.25
LANES = 128
SUBLANES = 8

VMEM = pl.BlockSpec(memory_space=pltpu.VMEM)
SMEM = pl.BlockSpec(memory_space=pltpu.SMEM)
PARAMS = pltpu.CompilerParams(vmem_limit_bytes=16 * 1024 * 1024)

INDEX = ((0, 0), (0, 1), (1, 0), (1, 1))


def comp(part, i, j):
    return part * 4 + i * 2 + j


def cadd(a, b):
    return (a[0] + b[0], a[1] + b[1])


def cmul(a, b):
    return (a[0] * b[0] - a[1] * b[1], a[0] * b[1] + a[1] * b[0])


def cmul_conj(a, b):
    return (a[0] * b[0] + a[1] * b[1], a[1] * b[0] - a[0] * b[1])


def mat_mul(a, b):
    return {(i, j): cadd(cmul(a[i, 0], b[0, j]), cmul(a[i, 1], b[1, j])) for i, j in INDEX}


def mat_mul_h(a, b):
    return {(i, j): cadd(cmul_conj(a[i, 0], b[j, 0]), cmul_conj(a[i, 1], b[j, 1])) for i, j in INDEX}


def mat_h_mul(a, b):
    return {(i, j): cadd(cmul_conj(b[0, j], a[0, i]), cmul_conj(b[1, j], a[1, i])) for i, j in INDEX}


def sq(a):
    return a[0] * a[0] + a[1] * a[1]


def split_dot(left, right, dims):
    high = left.astype(jnp.bfloat16)
    low = (left - high.astype(jnp.float32)).astype(jnp.bfloat16)
    both = jnp.concatenate([high, low], axis=0)
    out = lax.dot_general(both, right, (dims, ((), ())), preferred_element_type=jnp.float32)
    return out[: left.shape[0]] + out[left.shape[0] :]


def fill_onehot(pairs_ref, onehot_ref):
    stations = onehot_ref.shape[0]
    baselines = pairs_ref.shape[1]
    for half in range(2):
        ids = pairs_ref[half : half + 1, :]
        for base in range(0, stations, LANES):
            station = lax.broadcasted_iota(jnp.int32, (LANES, baselines), 0) + base
            hit = jnp.where(station == ids, 1.0, 0.0).astype(jnp.bfloat16)
            onehot_ref[base : base + LANES, half * baselines : (half + 1) * baselines] = hit


def read_rows(ref, dirs, k, base, width):
    def one(part, i, j):
        row = comp(part, i, j) * dirs + k
        return jnp.broadcast_to(ref[row : row + 1, base : base + width], (SUBLANES, width))

    return {(i, j): (one(0, i, j), one(1, i, j)) for i, j in INDEX}


def native_to_rows(block, dirs, store):
    for k in range(dirs):
        for part in range(2):
            for i in range(2):
                value = block(k, part, i)
                for j in range(2):
                    store(comp(part, i, j) * dirs + k, value[j : j + 1, :])


def prepare_kernel(basis_ref, dual_ref, coeffs_ref, dual_out_ref, known_ref):
    terms, dirs = coeffs_ref.shape[:2]

    def put(ref):
        def store(row, value):
            ref[row : row + 1, :] = value

        return store

    def known(k, part, i):
        total = coeffs_ref[0, k, part, i] * basis_ref[0, 0]
        for m in range(1, terms):
            total = total + coeffs_ref[m, k, part, i] * basis_ref[0, m]
        return RHO * total - dual_ref[k, part, i]

    native_to_rows(lambda k, part, i: dual_ref[k, part, i], dirs, put(dual_out_ref))
    native_to_rows(known, dirs, put(known_ref))


def model_body(parity_ref, jones, onehot_ref, coher_ref, gathered_ref, mine_ref, other_ref):
    dirs = coher_ref.shape[0]
    times, baselines = coher_ref.shape[-2:]
    gathered_ref[...] = split_dot(jones, onehot_ref[...], ((1,), (0,)))
    first = parity_ref[0, 0] == 0
    for base in range(0, baselines, LANES):
        lanes = slice(base, base + LANES)
        for time in range(0, times, SUBLANES):
            rows = slice(time, time + SUBLANES)
            total = None
            for k in range(dirs):
                jones_p = read_rows(gathered_ref, dirs, k, base, LANES)
                jones_q = read_rows(gathered_ref, dirs, k, baselines + base, LANES)
                coher = {(i, j): tuple(coher_ref[k, part, i, j, rows, lanes] for part in range(2)) for i, j in INDEX}
                model = mat_mul(jones_p, mat_mul_h(coher, jones_q))
                total = model if total is None else {ij: cadd(total[ij], model[ij]) for ij in INDEX}
            for i, j in INDEX:
                real, imag = total[i, j]
                mine_ref[i, j, rows, lanes] = jnp.where(first, real, imag)
                other_ref[i, j, rows, lanes] = jnp.where(first, imag, real)


def first_model_kernel(
    parity_ref, jones_ref, pairs_ref, coher_ref, gathered_ref, mine_ref, other_ref, onehot_ref, rows_ref
):
    fill_onehot(pairs_ref, onehot_ref)

    def store(row, value):
        rows_ref[row : row + 1, :] = value

    native_to_rows(lambda k, part, i: jones_ref[k, part, i], coher_ref.shape[0], store)
    model_body(parity_ref, rows_ref[...], onehot_ref, coher_ref, gathered_ref, mine_ref, other_ref)


def model_kernel(parity_ref, jones_ref, pairs_ref, coher_ref, gathered_ref, mine_ref, other_ref, onehot_ref):
    fill_onehot(pairs_ref, onehot_ref)
    model_body(parity_ref, jones_ref[...], onehot_ref, coher_ref, gathered_ref, mine_ref, other_ref)


def sums_kernel(
    parity_ref, gathered_ref, pairs_ref, coher_ref, vis_ref, mine_ref, other_ref, right_ref, inverse_ref,
    onehot_ref, left_ref,
):
    dirs = coher_ref.shape[0]
    times, baselines = coher_ref.shape[-2:]
    fill_onehot(pairs_ref, onehot_ref)
    first = parity_ref[0, 0] == 0
    for base in range(0, baselines, LANES):
        lanes = slice(base, base + LANES)
        resid = []
        for time in range(0, times, SUBLANES):
            rows = slice(time, time + SUBLANES)
            piece = {}
            for i, j in INDEX:
                mine = mine_ref[i, j, rows, lanes]
                other = other_ref[i, j, rows, lanes]
                piece[i, j] = (
                    vis_ref[0, i, j, rows, lanes] - jnp.where(first, mine, other),
                    vis_ref[1, i, j, rows, lanes] - jnp.where(first, other, mine),
                )
            resid.append(piece)
        for k in range(dirs):
            jones_p = read_rows(gathered_ref, dirs, k, base, LANES)
            jones_q = read_rows(gathered_ref, dirs, k, baselines + base, LANES)
            sums = None
            for index, time in enumerate(range(0, times, SUBLANES)):
                rows = slice(time, time + SUBLANES)
                coher = {(i, j): tuple(coher_ref[k, part, i, j, rows, lanes] for part in range(2)) for i, j in INDEX}
                along = mat_mul_h(coher, jones_q)
                ahead = mat_mul(jones_p, coher)
                right_p = mat_mul_h(resid[index], along)
                right_q = mat_h_mul(resid[index], ahead)
                cross_p = cadd(cmul_conj(along[0, 0], along[1, 0]), cmul_conj(along[0, 1], along[1, 1]))
                cross_q = cadd(cmul_conj(ahead[0, 1], ahead[0, 0]), cmul_conj(ahead[1, 1], ahead[1, 0]))
                terms_p = [right_p[ij][part] for part in range(2) for ij in INDEX] + [
                    sq(along[0, 0]) + sq(along[0, 1]),
                    sq(along[1, 0]) + sq(along[1, 1]),
                    cross_p[0],
                    cross_p[1],
                ]
                terms_q = [right_q[ij][part] for part in range(2) for ij in INDEX] + [
                    sq(ahead[0, 0]) + sq(ahead[1, 0]),
                    sq(ahead[0, 1]) + sq(ahead[1, 1]),
                    cross_q[0],
                    cross_q[1],
                ]
                terms = terms_p + terms_q
                sums = terms if sums is None else [a + b for a, b in zip(sums, terms)]
            for at, term in enumerate(sums):
                row = (at % 12) * dirs + k
                offset = base + (at // 12) * baselines
                left_ref[row : row + 1, offset : offset + LANES] = jnp.sum(term, axis=0, keepdims=True)

    def group(ref, at):
        return ref[at * dirs : (at + 1) * dirs, :]

    jones = {(i, j): (group(gathered_ref, comp(0, i, j)), group(gathered_ref, comp(1, i, j))) for i, j in INDEX}
    diag0, diag1 = group(left_ref, 8), group(left_ref, 9)
    off = (group(left_ref, 10), group(left_ref, 11))
    off_c = (off[0], -off[1])
    for i in range(2):
        left, right = jones[i, 0], jones[i, 1]
        col0 = cadd((left[0] * diag0, left[1] * diag0), cmul(right, off_c))
        col1 = cadd(cmul(left, off), (right[0] * diag1, right[1] * diag1))
        for j, col in ((0, col0), (1, col1)):
            for part in range(2):
                at = comp(part, i, j) * dirs
                left_ref[at : at + dirs, :] = left_ref[at : at + dirs, :] + col[part]

    sums = split_dot(left_ref[...], onehot_ref[...], ((1,), (1,)))
    right_ref[...] = sums[: 8 * dirs]
    m00 = sums[8 * dirs : 9 * dirs] + RHO
    m11 = sums[9 * dirs : 10 * dirs] + RHO
    m01 = (sums[10 * dirs : 11 * dirs], sums[11 * dirs : 12 * dirs])
    scale = 1.0 / (m00 * m11 - sq(m01))
    inverse_ref[0:dirs, :] = m11 * scale
    inverse_ref[dirs : 2 * dirs, :] = m00 * scale
    inverse_ref[2 * dirs : 3 * dirs, :] = -m01[0] * scale
    inverse_ref[3 * dirs :, :] = -m01[1] * scale


def solve(right_ref, inverse_ref, known, dirs):
    i00, i11, re01, im01 = (inverse_ref[at * dirs : (at + 1) * dirs, :] for at in range(4))
    i01, i10 = (re01, im01), (re01, -im01)
    out = {}
    for i in range(2):
        n = []
        for j in range(2):
            at = [comp(part, i, j) * dirs for part in range(2)]
            n.append(tuple(right_ref[a : a + dirs, :] + known(a) for a in at))
        out[i, 0] = cadd((n[0][0] * i00, n[0][1] * i00), cmul(n[1], i10))
        out[i, 1] = cadd(cmul(n[0], i01), (n[1][0] * i11, n[1][1] * i11))
    return out


def store_chunks(ref, a, value):
    width = ref.shape[2]
    for chunk in range(ref.shape[0]):
        ref[chunk, a : a + value.shape[0], :] = value[:, chunk * width : (chunk + 1) * width]


def store_shared(ref, a, value):
    if len(ref.shape) == 3:
        store_chunks(ref, a, value)
    else:
        ref[a : a + value.shape[0], :] = value


def first_update_kernel(basis_ref, right_ref, inverse_ref, known_ref, dual_ref, jones_ref, shared_ref):
    dirs = inverse_ref.shape[0] // 4
    out = solve(right_ref, inverse_ref, lambda a: known_ref[a : a + dirs, :], dirs)
    for (i, j), parts in out.items():
        for part in range(2):
            a = comp(part, i, j) * dirs
            jones_ref[a : a + dirs, :] = parts[part]
            store_shared(shared_ref, a, parts[part] + dual_ref[a : a + dirs, :] * (1.0 / RHO))
    if len(shared_ref.shape) == 3:
        rows, width = 8 * dirs, shared_ref.shape[2]
        terms = basis_ref.shape[1]
        for chunk in range(shared_ref.shape[0]):
            shared_ref[chunk, rows:, :] = jnp.zeros((shared_ref.shape[1] - rows, width), jnp.float32)
            shared_ref[chunk, rows : rows + 1, :terms] = basis_ref[...]


def advance_dual(consensus_ref, dual_ref, before_ref, dual_out_ref, dirs):
    def consensus(a):
        if len(consensus_ref.shape) == 2:
            return consensus_ref[a : a + dirs, :]
        pieces = [consensus_ref[chunk, a : a + dirs, :] for chunk in range(consensus_ref.shape[0])]
        return jnp.concatenate(pieces, axis=1)

    known = {}
    for a in range(0, 8 * dirs, dirs):
        value = consensus(a)
        dual = dual_ref[a : a + dirs, :] + RHO * (before_ref[a : a + dirs, :] - value)
        dual_out_ref[a : a + dirs, :] = dual
        known[a] = RHO * value - dual
    return known


def update_kernel(
    right_ref, inverse_ref, consensus_ref, dual_ref, before_ref, jones_ref, shared_ref, dual_out_ref
):
    dirs = inverse_ref.shape[0] // 4
    known = advance_dual(consensus_ref, dual_ref, before_ref, dual_out_ref, dirs)
    out = solve(right_ref, inverse_ref, known.get, dirs)
    for (i, j), parts in out.items():
        for part in range(2):
            a = comp(part, i, j) * dirs
            jones_ref[a : a + dirs, :] = parts[part]
            store_shared(shared_ref, a, parts[part] + dual_out_ref[a : a + dirs, :] * (1.0 / RHO))


def last_update_kernel(
    right_ref, inverse_ref, consensus_ref, dual_ref, before_ref, jones_ref, shared_ref, dual_out_ref, rows_ref
):
    dirs = inverse_ref.shape[0] // 4
    known = advance_dual(consensus_ref, dual_ref, before_ref, rows_ref, dirs)
    out = solve(right_ref, inverse_ref, known.get, dirs)
    for (i, j), parts in out.items():
        for part in range(2):
            a = comp(part, i, j) * dirs
            dual = rows_ref[a : a + dirs, :]
            shared = parts[part] + dual * (1.0 / RHO)
            for k in range(dirs):
                jones_ref[k, part, i, j : j + 1, :] = parts[part][k : k + 1, :]
                shared_ref[k, part, i, j : j + 1, :] = shared[k : k + 1, :]
                dual_out_ref[k, part, i, j : j + 1, :] = dual[k : k + 1, :]


def mix(matrix, values):
    out = []
    for g in range(matrix.shape[0]):
        total = None
        for f, value in enumerate(values):
            weight = jnp.broadcast_to(matrix[g : g + 1, f : f + 1], value.shape[-2:])
            total = weight * value if total is None else total + weight * value
        out.append(total)
    return out


def first_mix_kernel(place_ref, shared_ref, out_ref, spread_ref, weights_ref):
    bands = shared_ref.shape[0]
    rows = out_ref.shape[1]
    terms = weights_ref.shape[0]
    hi = lax.Precision.HIGHEST
    basis = jnp.concatenate([shared_ref[f, rows : rows + 1, :terms] for f in range(bands)], axis=0)
    gram = lax.dot_general(basis, basis, (((0,), (0,)), ((), ())), precision=hi, preferred_element_type=jnp.float32)
    row = lax.broadcasted_iota(jnp.int32, (terms, terms), 0)
    col = lax.broadcasted_iota(jnp.int32, (terms, terms), 1)
    gram = gram + jnp.where(row == col, RIDGE * bands, 0.0)
    inverse = jnp.where(row == col, 1.0, 0.0)
    for t in range(terms):
        scale = 1.0 / gram[t : t + 1, t : t + 1]
        g_row = gram[t : t + 1, :] * scale
        i_row = inverse[t : t + 1, :] * scale
        factor = gram[:, t : t + 1]
        here = row == t
        gram = jnp.where(here, g_row, gram - factor * g_row)
        inverse = jnp.where(here, i_row, inverse - factor * i_row)
    weights = lax.dot_general(inverse, basis, (((1,), (1,)), ((), ())), precision=hi, preferred_element_type=jnp.float32)
    spread = jnp.dot(basis, weights, precision=hi, preferred_element_type=jnp.float32)
    spread_ref[...] = spread
    for g, value in enumerate(mix(spread, [shared_ref[f, :rows, :] for f in range(bands)])):
        out_ref[g] = value
    band = lax.broadcasted_iota(jnp.int32, (bands, bands), 0)
    slot = lax.broadcasted_iota(jnp.int32, (bands, bands), 1)
    step = (slot + 1) // 2
    spot = lax.rem(place_ref[0, 0] + jnp.where(slot % 2 == 1, -step, step) + 2 * bands, bands)
    source = jnp.where(spot < bands // 2, 2 * spot, 2 * (bands - 1 - spot) + 1)
    chosen = jnp.where(source == band, 1.0, 0.0)
    weights_ref[...] = jnp.dot(weights, chosen, precision=hi, preferred_element_type=jnp.float32)


def mix_kernel(spread_ref, shared_ref, out_ref):
    for g, value in enumerate(mix(spread_ref[...], [shared_ref[f] for f in range(shared_ref.shape[0])])):
        out_ref[g] = value


def final_kernel(weights_ref, basis_ref, jones_ref, dual_ref, *refs):
    shared_refs, (coeffs_ref, dual_out_ref) = refs[:-2], refs[-2:]
    dirs = jones_ref.shape[0]
    half = dirs // 2
    weights = weights_ref[...]
    for k in range(dirs):
        for part in range(2):
            for i in range(2):
                values = [ref[k, part, i] for ref in shared_refs[:-2]]
                values.append(shared_refs[-2][k, part, i] if k < half else shared_refs[-1][k - half, part, i])
                consensus = None
                for m, value in enumerate(mix(weights, values)):
                    coeffs_ref[m, k, part, i] = value
                    share = value * basis_ref[0, m]
                    consensus = share if consensus is None else consensus + share
                dual_out_ref[k, part, i] = dual_ref[k, part, i] + RHO * (jones_ref[k, part, i] - consensus)


def struct(*shape, dtype=jnp.float32):
    return jax.ShapeDtypeStruct(shape, dtype)


def call(kernel, out_shape, scalars, args, scratch=()):
    many = isinstance(out_shape, (tuple, list))
    return pl.pallas_call(
        kernel,
        out_shape=out_shape,
        in_specs=[SMEM if at < scalars else VMEM for at in range(len(args))],
        out_specs=tuple(VMEM for _ in out_shape) if many else VMEM,
        scratch_shapes=list(scratch),
        compiler_params=PARAMS,
    )(*args)


def swap(value, axis, bit):
    size = lax.axis_size(axis)
    return lax.ppermute(value, axis, [(i, i ^ bit) for i in range(size)])


def sum_over_dir(mine, other):
    size = lax.axis_size("dir")
    mine = mine + swap(other, "dir", 1)
    bit = 2
    while bit < size:
        mine = mine + swap(mine, "dir", bit)
        bit *= 2
    return mine, swap(mine, "dir", 1)


def ring_place(size):
    at = lax.axis_index("band")
    return jnp.where(at % 2 == 0, at // 2, size - 1 - at // 2).astype(jnp.int32).reshape(1, 1)


def ring_gather(value):
    size = lax.axis_size("band")
    order = list(range(0, size, 2)) + list(range(size - 1, 0, -2))
    ahead = [(order[i], order[(i + 1) % size]) for i in range(size)]
    behind = [(b, a) for a, b in ahead]
    values = [value]
    up = down = value
    for step in range(1, (size - 1) // 2 + 1):
        up = lax.ppermute(up, "band", ahead)
        down = lax.ppermute(down, "band", behind)
        values += [up, down]
    half = value.shape[0] // 2
    return values + [lax.ppermute(up[:half], "band", ahead), lax.ppermute(down[half:], "band", behind)]


def reduce_bands(shared, row, factor):
    sums = lax.psum(row.reshape((-1,) + (1,) * shared.ndim) * shared[None], "band")
    flat = sums.reshape(sums.shape[0], -1)
    return jax.scipy.linalg.cho_solve((factor, True), flat).reshape(sums.shape)


def local(visibilities, coherencies, jones_start, dual_start, consensus_start, freq_basis, pairs):
    row = freq_basis[0]
    terms = row.shape[0]
    bands = lax.axis_size("band")
    vis, coher = visibilities[0], coherencies[0]
    native = jones_start.shape[1:]
    dirs, stations = native[0], native[-1]
    times, baselines = coher.shape[-2:]
    rows = 8 * dirs
    parity = (lax.axis_index("dir") % 2).astype(jnp.int32).reshape(1, 1)
    chunked = stations % (bands * LANES) == 0 and bands % 2 == 0 and dirs % 2 == 0
    hi = lax.Precision.HIGHEST
    half = struct(2, 2, times, baselines)
    flat = struct(rows, stations)
    onehot = pltpu.VMEM((stations, 2 * baselines), jnp.bfloat16)
    left = pltpu.VMEM((12 * dirs, 2 * baselines), jnp.float32)
    in_rows = pltpu.VMEM((rows, stations), jnp.float32)
    model_out = (struct(rows, 2 * baselines), half, half)

    if not chunked:
        gram = lax.psum(row[:, None] * row[None, :], "band") + RIDGE * bands * jnp.eye(terms, dtype=jnp.float32)
        factor = jnp.linalg.cholesky(gram)

    jones = jones_start[0]
    for turn in range(ITERS):
        last = turn == ITERS - 1
        gathered, mine, other = call(
            model_kernel if turn else first_model_kernel, model_out, 1, (parity, jones, pairs, coher),
            [onehot] if turn else [onehot, in_rows],
        )
        if turn == 0:
            dual, known = call(prepare_kernel, (flat, flat), 1, (freq_basis, dual_start[0], consensus_start))
        mine, other = sum_over_dir(mine, other)
        right, inverse = call(
            sums_kernel, (flat, struct(4 * dirs, stations)), 1,
            (parity, gathered, pairs, coher, vis, mine, other), [onehot, left],
        )
        if turn == 0:
            shape = struct(bands, rows + SUBLANES, stations // bands) if chunked else flat
            jones, shared = call(
                first_update_kernel, (flat, shape), 0, (freq_basis, right, inverse, known, dual)
            )
        elif not last:
            shape = struct(bands, rows, stations // bands) if chunked else flat
            jones, shared, dual = call(
                update_kernel, (flat, shape, flat), 0, (right, inverse, consensus, dual, jones)
            )
        else:
            jones, shared, dual = call(
                last_update_kernel, (struct(*native),) * 3, 0, (right, inverse, consensus, dual, jones), [in_rows]
            )
            break
        if chunked:
            shared = lax.all_to_all(shared, "band", 0, 0)
            mixed = struct(bands, rows, stations // bands)
            if turn == 0:
                mixed, spread, weights = call(
                    first_mix_kernel, (mixed, struct(bands, bands), struct(terms, bands)), 1,
                    (ring_place(bands), shared),
                )
            else:
                mixed = call(mix_kernel, mixed, 0, (spread, shared))
            consensus = lax.all_to_all(mixed, "band", 0, 0)
        else:
            coeffs = reduce_bands(shared, row, factor)
            consensus = jnp.tensordot(row, coeffs, axes=(0, 0), precision=hi)
    if chunked:
        values = ring_gather(shared)

        def kernel(weights_ref, basis_ref, *refs):
            final_kernel(weights_ref, basis_ref, *refs)

        coeffs, dual = pl.pallas_call(
            kernel,
            out_shape=(struct(terms, *native), struct(*native)),
            in_specs=[VMEM, SMEM] + [VMEM] * (2 + len(values)),
            out_specs=(VMEM, VMEM),
            compiler_params=PARAMS,
        )(weights, freq_basis, jones, dual, *values)
    else:
        coeffs = reduce_bands(shared, row, factor)
        dual = dual + RHO * (jones - jnp.tensordot(row, coeffs, axes=(0, 0), precision=hi))
    return jones[None], dual[None], coeffs


def solution(mesh):
    in_specs = (
        P("band", None, None, None, None, None),
        P("band", "dir", None, None, None, None, None),
        P("band", "dir", None, None, None, None),
        P("band", "dir", None, None, None, None),
        P(None, "dir", None, None, None, None),
        P("band", None),
        P(),
    )
    out_specs = (
        P("band", "dir", None, None, None, None),
        P("band", "dir", None, None, None, None),
        P(None, "dir", None, None, None, None),
    )
    return jax.shard_map(local, mesh=mesh, in_specs=in_specs, out_specs=out_specs, check_vma=False)
```

```python
import jax
import jax.numpy as jnp
from jax import lax
from jax.experimental import pallas as pl
from jax.experimental.pallas import tpu as pltpu
from jax.sharding import PartitionSpec as P

ITERS = 3
RHO = 5.0
RIDGE = 0.25
LANES = 128
SUBLANES = 8

VMEM = pl.BlockSpec(memory_space=pltpu.VMEM)
SMEM = pl.BlockSpec(memory_space=pltpu.SMEM)
PARAMS = pltpu.CompilerParams(vmem_limit_bytes=16 * 1024 * 1024)

INDEX = ((0, 0), (0, 1), (1, 0), (1, 1))


def comp(part, i, j):
    return part * 4 + i * 2 + j


def cadd(a, b):
    return (a[0] + b[0], a[1] + b[1])


def cmul(a, b):
    return (a[0] * b[0] - a[1] * b[1], a[0] * b[1] + a[1] * b[0])


def cmul_conj(a, b):
    return (a[0] * b[0] + a[1] * b[1], a[1] * b[0] - a[0] * b[1])


def mat_mul(a, b):
    return {(i, j): cadd(cmul(a[i, 0], b[0, j]), cmul(a[i, 1], b[1, j])) for i, j in INDEX}


def mat_mul_h(a, b):
    return {(i, j): cadd(cmul_conj(a[i, 0], b[j, 0]), cmul_conj(a[i, 1], b[j, 1])) for i, j in INDEX}


def mat_h_mul(a, b):
    return {(i, j): cadd(cmul_conj(b[0, j], a[0, i]), cmul_conj(b[1, j], a[1, i])) for i, j in INDEX}


def sq(a):
    return a[0] * a[0] + a[1] * a[1]


def split_dot(left, right, dims):
    high = left.astype(jnp.bfloat16)
    low = (left - high.astype(jnp.float32)).astype(jnp.bfloat16)
    both = jnp.concatenate([high, low], axis=0)
    out = lax.dot_general(both, right, (dims, ((), ())), preferred_element_type=jnp.float32)
    return out[: left.shape[0]] + out[left.shape[0] :]


def fill_onehot(pairs_ref, onehot_ref):
    stations = onehot_ref.shape[0]
    baselines = pairs_ref.shape[1]
    for half in range(2):
        ids = pairs_ref[half : half + 1, :]
        for base in range(0, stations, LANES):
            station = lax.broadcasted_iota(jnp.int32, (LANES, baselines), 0) + base
            hit = jnp.where(station == ids, 1.0, 0.0).astype(jnp.bfloat16)
            onehot_ref[base : base + LANES, half * baselines : (half + 1) * baselines] = hit


def read_rows(ref, dirs, k, base, width):
    def one(part, i, j):
        row = comp(part, i, j) * dirs + k
        return jnp.broadcast_to(ref[row : row + 1, base : base + width], (SUBLANES, width))

    return {(i, j): (one(0, i, j), one(1, i, j)) for i, j in INDEX}


def native_to_rows(block, dirs, store):
    for k in range(dirs):
        for part in range(2):
            for i in range(2):
                value = block(k, part, i)
                for j in range(2):
                    store(comp(part, i, j) * dirs + k, value[j : j + 1, :])


def store_chunks(ref, row, value):
    width = ref.shape[2]
    for chunk in range(ref.shape[0]):
        ref[chunk, row : row + value.shape[0], :] = value[:, chunk * width : (chunk + 1) * width]


def prepare_kernel(basis_ref, dual_ref, coeffs_ref, known_ref, lag_ref):
    terms, dirs = coeffs_ref.shape[:2]

    def known(k, part, i):
        total = coeffs_ref[0, k, part, i] * basis_ref[0, 0]
        for m in range(1, terms):
            total = total + coeffs_ref[m, k, part, i] * basis_ref[0, m]
        return RHO * total - dual_ref[k, part, i]

    native_to_rows(known, dirs, lambda row, value: store_chunks(known_ref, row, value))
    native_to_rows(
        lambda k, part, i: dual_ref[k, part, i] * (1.0 / RHO), dirs,
        lambda row, value: store_chunks(lag_ref, row, value),
    )


def model_body(parity_ref, jones, onehot_ref, coher_ref, gathered_ref, mine_ref, other_ref):
    dirs = coher_ref.shape[0]
    times, baselines = coher_ref.shape[-2:]
    gathered_ref[...] = split_dot(jones, onehot_ref[...], ((1,), (0,)))
    first = parity_ref[0, 0] == 0
    for base in range(0, baselines, LANES):
        lanes = slice(base, base + LANES)
        for time in range(0, times, SUBLANES):
            rows = slice(time, time + SUBLANES)
            total = None
            for k in range(dirs):
                jones_p = read_rows(gathered_ref, dirs, k, base, LANES)
                jones_q = read_rows(gathered_ref, dirs, k, baselines + base, LANES)
                coher = {(i, j): tuple(coher_ref[k, part, i, j, rows, lanes] for part in range(2)) for i, j in INDEX}
                model = mat_mul(jones_p, mat_mul_h(coher, jones_q))
                total = model if total is None else {ij: cadd(total[ij], model[ij]) for ij in INDEX}
            for i, j in INDEX:
                real, imag = total[i, j]
                mine_ref[i, j, rows, lanes] = jnp.where(first, real, imag)
                other_ref[i, j, rows, lanes] = jnp.where(first, imag, real)


def first_model_kernel(
    parity_ref, jones_ref, pairs_ref, coher_ref, gathered_ref, mine_ref, other_ref, onehot_ref, rows_ref
):
    fill_onehot(pairs_ref, onehot_ref)

    def store(row, value):
        rows_ref[row : row + 1, :] = value

    native_to_rows(lambda k, part, i: jones_ref[k, part, i], coher_ref.shape[0], store)
    model_body(parity_ref, rows_ref[...], onehot_ref, coher_ref, gathered_ref, mine_ref, other_ref)


def model_kernel(parity_ref, jones_ref, pairs_ref, coher_ref, gathered_ref, mine_ref, other_ref, onehot_ref):
    fill_onehot(pairs_ref, onehot_ref)
    model_body(parity_ref, jones_ref[...], onehot_ref, coher_ref, gathered_ref, mine_ref, other_ref)


def sums_kernel(
    parity_ref, gathered_ref, pairs_ref, coher_ref, vis_ref, mine_ref, other_ref, sums_ref, onehot_ref, left_ref
):
    dirs = coher_ref.shape[0]
    times, baselines = coher_ref.shape[-2:]
    fill_onehot(pairs_ref, onehot_ref)
    first = parity_ref[0, 0] == 0
    for base in range(0, baselines, LANES):
        lanes = slice(base, base + LANES)
        resid = []
        for time in range(0, times, SUBLANES):
            rows = slice(time, time + SUBLANES)
            piece = {}
            for i, j in INDEX:
                mine = mine_ref[i, j, rows, lanes]
                other = other_ref[i, j, rows, lanes]
                piece[i, j] = (
                    vis_ref[0, i, j, rows, lanes] - jnp.where(first, mine, other),
                    vis_ref[1, i, j, rows, lanes] - jnp.where(first, other, mine),
                )
            resid.append(piece)
        for k in range(dirs):
            jones_p = read_rows(gathered_ref, dirs, k, base, LANES)
            jones_q = read_rows(gathered_ref, dirs, k, baselines + base, LANES)
            sums = None
            for index, time in enumerate(range(0, times, SUBLANES)):
                rows = slice(time, time + SUBLANES)
                coher = {(i, j): tuple(coher_ref[k, part, i, j, rows, lanes] for part in range(2)) for i, j in INDEX}
                along = mat_mul_h(coher, jones_q)
                ahead = mat_mul(jones_p, coher)
                right_p = mat_mul_h(resid[index], along)
                right_q = mat_h_mul(resid[index], ahead)
                cross_p = cadd(cmul_conj(along[0, 0], along[1, 0]), cmul_conj(along[0, 1], along[1, 1]))
                cross_q = cadd(cmul_conj(ahead[0, 1], ahead[0, 0]), cmul_conj(ahead[1, 1], ahead[1, 0]))
                terms_p = [right_p[ij][part] for part in range(2) for ij in INDEX] + [
                    sq(along[0, 0]) + sq(along[0, 1]),
                    sq(along[1, 0]) + sq(along[1, 1]),
                    cross_p[0],
                    cross_p[1],
                ]
                terms_q = [right_q[ij][part] for part in range(2) for ij in INDEX] + [
                    sq(ahead[0, 0]) + sq(ahead[1, 0]),
                    sq(ahead[0, 1]) + sq(ahead[1, 1]),
                    cross_q[0],
                    cross_q[1],
                ]
                terms = terms_p + terms_q
                sums = terms if sums is None else [a + b for a, b in zip(sums, terms)]
            for at, term in enumerate(sums):
                row = (at % 12) * dirs + k
                offset = base + (at // 12) * baselines
                left_ref[row : row + 1, offset : offset + LANES] = jnp.sum(term, axis=0, keepdims=True)

    def group(ref, at):
        return ref[at * dirs : (at + 1) * dirs, :]

    jones = {(i, j): (group(gathered_ref, comp(0, i, j)), group(gathered_ref, comp(1, i, j))) for i, j in INDEX}
    diag0, diag1 = group(left_ref, 8), group(left_ref, 9)
    off = (group(left_ref, 10), group(left_ref, 11))
    off_c = (off[0], -off[1])
    for i in range(2):
        left, right = jones[i, 0], jones[i, 1]
        col0 = cadd((left[0] * diag0, left[1] * diag0), cmul(right, off_c))
        col1 = cadd(cmul(left, off), (right[0] * diag1, right[1] * diag1))
        for j, col in ((0, col0), (1, col1)):
            for part in range(2):
                at = comp(part, i, j) * dirs
                left_ref[at : at + dirs, :] = left_ref[at : at + dirs, :] + col[part]

    sums = split_dot(left_ref[...], onehot_ref[...], ((1,), (1,)))
    store_chunks(sums_ref, 0, sums[: 8 * dirs])
    m00 = sums[8 * dirs : 9 * dirs] + RHO
    m11 = sums[9 * dirs : 10 * dirs] + RHO
    m01 = (sums[10 * dirs : 11 * dirs], sums[11 * dirs : 12 * dirs])
    scale = 1.0 / (m00 * m11 - sq(m01))
    store_chunks(sums_ref, 8 * dirs, m11 * scale)
    store_chunks(sums_ref, 9 * dirs, m00 * scale)
    store_chunks(sums_ref, 10 * dirs, -m01[0] * scale)
    store_chunks(sums_ref, 11 * dirs, -m01[1] * scale)


def solve(sums, known, dirs):
    i00, i11, re01, im01 = (sums(at * dirs) for at in range(8, 12))
    i01, i10 = (re01, im01), (re01, -im01)
    out = {}
    for i in range(2):
        n = []
        for j in range(2):
            at = [comp(part, i, j) * dirs for part in range(2)]
            n.append(tuple(sums(a) + known(a) for a in at))
        left = cadd((n[0][0] * i00, n[0][1] * i00), cmul(n[1], i10))
        right = cadd(cmul(n[0], i01), (n[1][0] * i11, n[1][1] * i11))
        for part in range(2):
            out[comp(part, i, 0) * dirs] = left[part]
            out[comp(part, i, 1) * dirs] = right[part]
    return out


def first_update_kernel(basis_ref, sums_ref, known_ref, lag_ref, jones_ref, unit_ref):
    dirs = sums_ref.shape[1] // 12
    chunks, rows, width = known_ref.shape
    terms = basis_ref.shape[1]
    for chunk in range(chunks):
        out = solve(
            lambda a: sums_ref[chunk, a : a + dirs, :], lambda a: known_ref[chunk, a : a + dirs, :], dirs
        )
        for a, value in out.items():
            jones_ref[a : a + dirs, chunk * width : (chunk + 1) * width] = value
            at = chunk * rows + a
            unit_ref[at : at + dirs, :] = value + lag_ref[chunk, a : a + dirs, :]
    unit_ref[chunks * rows :, :] = jnp.zeros((SUBLANES, width), jnp.float32)
    unit_ref[chunks * rows : chunks * rows + 1, :terms] = basis_ref[...]


def solve_next(sums, consensus, before, dirs):
    out = solve(sums, lambda a: RHO * (2.0 * consensus(a) - before(a)), dirs)
    return out, {a: value + (before(a) - consensus(a)) for a, value in out.items()}


def solve_chunk(chunk, sums_ref, consensus_ref, before_ref):
    dirs = sums_ref.shape[1] // 12

    def rows(ref):
        return lambda a: ref[chunk, a : a + dirs, :]

    return solve_next(rows(sums_ref), rows(consensus_ref), rows(before_ref), dirs)


def update_kernel(sums_ref, consensus_ref, before_ref, jones_ref, shared_ref):
    dirs, width = sums_ref.shape[1] // 12, sums_ref.shape[2]
    for chunk in range(sums_ref.shape[0]):
        jones, shared = solve_chunk(chunk, sums_ref, consensus_ref, before_ref)
        for a in jones:
            jones_ref[a : a + dirs, chunk * width : (chunk + 1) * width] = jones[a]
            shared_ref[chunk, a : a + dirs, :] = shared[a]


def store_native(chunk, width, dirs, rows, ref):
    for part in range(2):
        for i, j in INDEX:
            value = rows[comp(part, i, j) * dirs]
            for k in range(dirs):
                ref[k, part, i, j : j + 1, chunk * width : (chunk + 1) * width] = value[k : k + 1, :]


def last_update_kernel(sums_ref, consensus_ref, before_ref, jones_ref, shared_ref):
    dirs, width = sums_ref.shape[1] // 12, sums_ref.shape[2]
    for chunk in range(sums_ref.shape[0]):
        jones, shared = solve_chunk(chunk, sums_ref, consensus_ref, before_ref)
        store_native(chunk, width, dirs, jones, jones_ref)
        store_native(chunk, width, dirs, shared, shared_ref)


def weighted(matrix, g, values):
    total = None
    for f, value in enumerate(values):
        weight = jnp.broadcast_to(matrix[g : g + 1, f : f + 1], value.shape[-2:])
        total = weight * value if total is None else total + weight * value
    return total


def gathered_update_kernel(sums_ref, *refs):
    units, (jones_ref, shared_ref, spread_ref, weights_ref) = refs[:-4], refs[-4:]
    own, tail = units[0], units[-1]
    dirs = sums_ref.shape[1] // 12
    chunks, _, width = sums_ref.shape
    rows = 8 * dirs
    terms = weights_ref.shape[0]
    bands = len(units) - 1
    hi = lax.Precision.HIGHEST
    at = chunks * rows
    start = own.shape[0] - tail.shape[0]
    basis = jnp.concatenate(
        [ref[at : at + 1, :terms] for ref in units[:-2]] + [tail[at - start : at - start + 1, :terms]], axis=0
    )
    gram = lax.dot_general(basis, basis, (((0,), (0,)), ((), ())), precision=hi, preferred_element_type=jnp.float32)
    row = lax.broadcasted_iota(jnp.int32, (terms, terms), 0)
    col = lax.broadcasted_iota(jnp.int32, (terms, terms), 1)
    gram = gram + jnp.where(row == col, RIDGE * bands, 0.0)
    inverse = jnp.where(row == col, 1.0, 0.0)
    for t in range(terms):
        scale = 1.0 / gram[t : t + 1, t : t + 1]
        g_row = gram[t : t + 1, :] * scale
        i_row = inverse[t : t + 1, :] * scale
        factor = gram[:, t : t + 1]
        here = row == t
        gram = jnp.where(here, g_row, gram - factor * g_row)
        inverse = jnp.where(here, i_row, inverse - factor * i_row)
    weights = lax.dot_general(inverse, basis, (((1,), (1,)), ((), ())), precision=hi, preferred_element_type=jnp.float32)
    spread = jnp.dot(basis, weights, precision=hi, preferred_element_type=jnp.float32)
    spread_ref[...] = spread
    weights_ref[...] = weights
    for chunk in range(chunks):
        jones, shared = solve_gathered(chunk, spread, sums_ref, units, rows)
        for a in jones:
            jones_ref[a : a + dirs, chunk * width : (chunk + 1) * width] = jones[a]
            shared_ref[chunk * rows + a : chunk * rows + a + dirs, :] = shared[a]


def solve_gathered(chunk, spread, sums_ref, units, rows):
    dirs = sums_ref.shape[1] // 12
    head, tail = units[-2:]
    base, start = chunk * rows, head.shape[0]
    values = [ref[base : base + rows, :] for ref in units[:-2]]
    values.append(head[base : base + rows, :] if base < start else tail[base - start : base - start + rows, :])
    consensus = weighted(spread, 0, values)
    return solve_next(
        lambda a: sums_ref[chunk, a : a + dirs, :],
        lambda a: consensus[a : a + dirs],
        lambda a: values[0][a : a + dirs],
        dirs,
    )


def gathered_last_kernel(spread_ref, sums_ref, *refs):
    units, (jones_ref, shared_ref) = refs[:-2], refs[-2:]
    dirs, width = sums_ref.shape[1] // 12, sums_ref.shape[2]
    spread = spread_ref[...]
    for chunk in range(sums_ref.shape[0]):
        jones, shared = solve_gathered(chunk, spread, sums_ref, units, 8 * dirs)
        store_native(chunk, width, dirs, jones, jones_ref)
        store_native(chunk, width, dirs, shared, shared_ref)


def final_kernel(weights_ref, basis_ref, *refs):
    shared_refs, (coeffs_ref, dual_ref) = refs[:-2], refs[-2:]
    dirs = dual_ref.shape[0]
    half = dirs // 2
    weights = weights_ref[...]
    for k in range(dirs):
        for part in range(2):
            for i in range(2):
                values = [ref[k, part, i] for ref in shared_refs[:-2]]
                values.append(shared_refs[-2][k, part, i] if k < half else shared_refs[-1][k - half, part, i])
                consensus = None
                for m in range(weights.shape[0]):
                    value = weighted(weights, m, values)
                    coeffs_ref[m, k, part, i] = value
                    share = value * basis_ref[0, m]
                    consensus = share if consensus is None else consensus + share
                dual_ref[k, part, i] = RHO * (values[0] - consensus)


def struct(*shape, dtype=jnp.float32):
    return jax.ShapeDtypeStruct(shape, dtype)


def call(kernel, out_shape, scalars, args, scratch=()):
    many = isinstance(out_shape, (tuple, list))
    return pl.pallas_call(
        kernel,
        out_shape=out_shape,
        in_specs=[SMEM if at < scalars else VMEM for at in range(len(args))],
        out_specs=tuple(VMEM for _ in out_shape) if many else VMEM,
        scratch_shapes=list(scratch),
        compiler_params=PARAMS,
    )(*args)


def swap(value, axis, bit):
    size = lax.axis_size(axis)
    return lax.ppermute(value, axis, [(i, i ^ bit) for i in range(size)])


def sum_over_dir(mine, other):
    size = lax.axis_size("dir")
    mine = mine + swap(other, "dir", 1)
    bit = 2
    while bit < size:
        mine = mine + swap(mine, "dir", bit)
        bit *= 2
    return mine, swap(mine, "dir", 1)


def ring_gather(value, half):
    size = lax.axis_size("band")
    order = list(range(0, size, 2)) + list(range(size - 1, 0, -2))
    ahead = [(order[i], order[(i + 1) % size]) for i in range(size)]
    behind = [(b, a) for a, b in ahead]
    values = [value]
    up = down = value
    for step in range(1, (size - 1) // 2 + 1):
        up = lax.ppermute(up, "band", ahead)
        down = lax.ppermute(down, "band", behind)
        values += [up, down]
    return values + [lax.ppermute(up[:half], "band", ahead), lax.ppermute(down[half:], "band", behind)]


def reduce_bands(shared, row, factor):
    sums = lax.psum(row.reshape((-1,) + (1,) * shared.ndim) * shared[None], "band")
    flat = sums.reshape(sums.shape[0], -1)
    return jax.scipy.linalg.cho_solve((factor, True), flat).reshape(sums.shape)


def local(visibilities, coherencies, jones_start, dual_start, consensus_start, freq_basis, pairs):
    row = freq_basis[0]
    terms = row.shape[0]
    bands = lax.axis_size("band")
    vis, coher = visibilities[0], coherencies[0]
    native = jones_start.shape[1:]
    dirs, stations = native[0], native[-1]
    times, baselines = coher.shape[-2:]
    rows = 8 * dirs
    parity = (lax.axis_index("dir") % 2).astype(jnp.int32).reshape(1, 1)
    chunked = stations % (bands * LANES) == 0 and bands % 2 == 0 and dirs % 2 == 0
    hi = lax.Precision.HIGHEST
    width = stations // bands if chunked else LANES
    chunks = stations // width
    half = struct(2, 2, times, baselines)
    flat = struct(rows, stations)
    spread_rows = struct(chunks, rows, width)
    onehot = pltpu.VMEM((stations, 2 * baselines), jnp.bfloat16)
    left = pltpu.VMEM((12 * dirs, 2 * baselines), jnp.float32)
    in_rows = pltpu.VMEM((rows, stations), jnp.float32)
    model_out = (struct(rows, 2 * baselines), half, half)

    if not chunked:
        gram = lax.psum(row[:, None] * row[None, :], "band") + RIDGE * bands * jnp.eye(terms, dtype=jnp.float32)
        factor = jnp.linalg.cholesky(gram)

    def model(jones, first=False):
        return call(
            first_model_kernel if first else model_kernel, model_out, 1, (parity, jones, pairs, coher),
            [onehot, in_rows] if first else [onehot],
        )

    def station_sums(gathered, mine, other):
        mine, other = sum_over_dir(mine, other)
        return call(
            sums_kernel, struct(chunks, 12 * dirs, width), 1,
            (parity, gathered, pairs, coher, vis, mine, other), [onehot, left],
        )

    def share(shared):
        coeffs = reduce_bands(shared, row, factor)
        return coeffs, jnp.tensordot(row, coeffs, axes=(0, 0), precision=hi)

    started = model(jones_start[0], True)
    known, lag = call(prepare_kernel, (spread_rows,) * 2, 1, (freq_basis, dual_start[0], consensus_start))
    jones, unit = call(
        first_update_kernel, (flat, struct(stations * rows // width + SUBLANES, width)), 0,
        (freq_basis, station_sums(*started), known, lag),
    )
    if chunked:
        half_rows = chunks // 2 * rows
        units = ring_gather(unit, half_rows)
        sums = station_sums(*model(jones))
        jones, unit, spread, weights = call(
            gathered_update_kernel,
            (flat, struct(chunks * rows, width), struct(bands, bands), struct(terms, bands)), 0, (sums, *units),
        )
        units = ring_gather(unit, half_rows)
        sums = station_sums(*model(jones))
        jones, shared = call(gathered_last_kernel, (struct(*native),) * 2, 0, (spread, sums, *units))
        values = ring_gather(shared, dirs // 2)
        coeffs, dual = pl.pallas_call(
            final_kernel,
            out_shape=(struct(terms, *native), struct(*native)),
            in_specs=[VMEM, SMEM] + [VMEM] * len(values),
            out_specs=(VMEM, VMEM),
            compiler_params=PARAMS,
        )(weights, freq_basis, *values)
    else:
        shared = unit[: chunks * rows].reshape(spread_rows.shape)
        for _ in range(ITERS - 2):
            consensus = share(shared)[1]
            sums = station_sums(*model(jones))
            jones, shared = call(update_kernel, (flat, spread_rows), 0, (sums, consensus, shared))
        consensus = share(shared)[1]
        sums = station_sums(*model(jones))
        jones, shared = call(last_update_kernel, (struct(*native),) * 2, 0, (sums, consensus, shared))
        coeffs, consensus = share(shared)
        dual = RHO * (shared - consensus)
    return jones[None], dual[None], coeffs


def solution(mesh):
    in_specs = (
        P("band", None, None, None, None, None),
        P("band", "dir", None, None, None, None, None),
        P("band", "dir", None, None, None, None),
        P("band", "dir", None, None, None, None),
        P(None, "dir", None, None, None, None),
        P("band", None),
        P(),
    )
    out_specs = (
        P("band", "dir", None, None, None, None),
        P("band", "dir", None, None, None, None),
        P(None, "dir", None, None, None, None),
    )
    return jax.shard_map(local, mesh=mesh, in_specs=in_specs, out_specs=out_specs, check_vma=False)
```

```python
import jax
import jax.numpy as jnp
from jax import lax
from jax.experimental import pallas as pl
from jax.experimental.pallas import tpu as pltpu
from jax.sharding import PartitionSpec as P

ITERS = 3
RHO = 5.0
RIDGE = 0.25
LANES = 128
SUBLANES = 8

VMEM = pl.BlockSpec(memory_space=pltpu.VMEM)
SMEM = pl.BlockSpec(memory_space=pltpu.SMEM)
HBM = pl.BlockSpec(memory_space=pltpu.HBM)
PARAMS = pltpu.CompilerParams(vmem_limit_bytes=16 * 1024 * 1024)

INDEX = ((0, 0), (0, 1), (1, 0), (1, 1))


def comp(part, i, j):
    return part * 4 + i * 2 + j


def cadd(a, b):
    return (a[0] + b[0], a[1] + b[1])


def cmul(a, b):
    return (a[0] * b[0] - a[1] * b[1], a[0] * b[1] + a[1] * b[0])


def cmul_conj(a, b):
    return (a[0] * b[0] + a[1] * b[1], a[1] * b[0] - a[0] * b[1])


def mat_mul(a, b):
    return {(i, j): cadd(cmul(a[i, 0], b[0, j]), cmul(a[i, 1], b[1, j])) for i, j in INDEX}


def mat_mul_h(a, b):
    return {(i, j): cadd(cmul_conj(a[i, 0], b[j, 0]), cmul_conj(a[i, 1], b[j, 1])) for i, j in INDEX}


def mat_h_mul(a, b):
    return {(i, j): cadd(cmul_conj(b[0, j], a[0, i]), cmul_conj(b[1, j], a[1, i])) for i, j in INDEX}


def sq(a):
    return a[0] * a[0] + a[1] * a[1]


def split_dot(left, right, dims):
    high = left.astype(jnp.bfloat16)
    low = (left - high.astype(jnp.float32)).astype(jnp.bfloat16)
    both = jnp.concatenate([high, low], axis=0)
    out = lax.dot_general(both, right, (dims, ((), ())), preferred_element_type=jnp.float32)
    return out[: left.shape[0]] + out[left.shape[0] :]


def fill_onehot(pairs_ref, onehot_ref):
    stations = onehot_ref.shape[0]
    baselines = pairs_ref.shape[1]
    for half in range(2):
        ids = pairs_ref[half : half + 1, :]
        for base in range(0, stations, LANES):
            station = lax.broadcasted_iota(jnp.int32, (LANES, baselines), 0) + base
            hit = jnp.where(station == ids, 1.0, 0.0).astype(jnp.bfloat16)
            onehot_ref[base : base + LANES, half * baselines : (half + 1) * baselines] = hit


def read_rows(ref, dirs, k, base, width):
    def one(part, i, j):
        row = comp(part, i, j) * dirs + k
        return jnp.broadcast_to(ref[row : row + 1, base : base + width], (SUBLANES, width))

    return {(i, j): (one(0, i, j), one(1, i, j)) for i, j in INDEX}


def native_to_rows(block, dirs, store):
    for k in range(dirs):
        for part in range(2):
            for i in range(2):
                value = block(k, part, i)
                for j in range(2):
                    store(comp(part, i, j) * dirs + k, value[j : j + 1, :])


def store_chunks(ref, row, value):
    width = ref.shape[2]
    for chunk in range(ref.shape[0]):
        ref[chunk, row : row + value.shape[0], :] = value[:, chunk * width : (chunk + 1) * width]


def prepare_kernel(basis_ref, dual_ref, coeffs_ref, known_ref, lag_ref):
    terms, dirs = coeffs_ref.shape[:2]

    def known(k, part, i):
        total = coeffs_ref[0, k, part, i] * basis_ref[0, 0]
        for m in range(1, terms):
            total = total + coeffs_ref[m, k, part, i] * basis_ref[0, m]
        return RHO * total - dual_ref[k, part, i]

    native_to_rows(known, dirs, lambda row, value: store_chunks(known_ref, row, value))
    native_to_rows(
        lambda k, part, i: dual_ref[k, part, i] * (1.0 / RHO), dirs,
        lambda row, value: store_chunks(lag_ref, row, value),
    )


def model_body(parity_ref, jones, onehot_ref, coher_ref, gathered_ref, mine_ref, other_ref):
    dirs = coher_ref.shape[0]
    times, baselines = coher_ref.shape[-2:]
    gathered_ref[...] = split_dot(jones, onehot_ref[...], ((1,), (0,)))
    first = parity_ref[0, 0] == 0
    for base in range(0, baselines, LANES):
        lanes = slice(base, base + LANES)
        for time in range(0, times, SUBLANES):
            rows = slice(time, time + SUBLANES)
            total = None
            for k in range(dirs):
                jones_p = read_rows(gathered_ref, dirs, k, base, LANES)
                jones_q = read_rows(gathered_ref, dirs, k, baselines + base, LANES)
                coher = {(i, j): tuple(coher_ref[k, part, i, j, rows, lanes] for part in range(2)) for i, j in INDEX}
                model = mat_mul(jones_p, mat_mul_h(coher, jones_q))
                total = model if total is None else {ij: cadd(total[ij], model[ij]) for ij in INDEX}
            for i, j in INDEX:
                real, imag = total[i, j]
                mine_ref[i, j, rows, lanes] = jnp.where(first, real, imag)
                other_ref[i, j, rows, lanes] = jnp.where(first, imag, real)


def first_model_kernel(
    parity_ref, jones_hbm, pairs_hbm, coher_hbm, gathered_ref, mine_ref, other_ref,
    onehot_ref, rows_ref, jones_ref, pairs_ref, coher_ref, sems,
):
    copies = [
        pltpu.make_async_copy(source, target, sems.at[at])
        for at, (source, target) in enumerate(
            ((pairs_hbm, pairs_ref), (jones_hbm, jones_ref), (coher_hbm, coher_ref))
        )
    ]
    for copy in copies:
        copy.start()
    copies[0].wait()
    fill_onehot(pairs_ref, onehot_ref)
    copies[1].wait()

    def store(row, value):
        rows_ref[row : row + 1, :] = value

    native_to_rows(lambda k, part, i: jones_ref[k, part, i], coher_ref.shape[0], store)
    copies[2].wait()
    model_body(parity_ref, rows_ref[...], onehot_ref, coher_ref, gathered_ref, mine_ref, other_ref)


def model_kernel(parity_ref, jones_ref, pairs_ref, coher_ref, gathered_ref, mine_ref, other_ref, onehot_ref):
    fill_onehot(pairs_ref, onehot_ref)
    model_body(parity_ref, jones_ref[...], onehot_ref, coher_ref, gathered_ref, mine_ref, other_ref)


def sums_kernel(
    parity_ref, gathered_ref, pairs_ref, coher_ref, vis_ref, mine_ref, other_ref, sums_ref, onehot_ref, left_ref
):
    dirs = coher_ref.shape[0]
    times, baselines = coher_ref.shape[-2:]
    fill_onehot(pairs_ref, onehot_ref)
    first = parity_ref[0, 0] == 0
    for base in range(0, baselines, LANES):
        lanes = slice(base, base + LANES)
        resid = []
        for time in range(0, times, SUBLANES):
            rows = slice(time, time + SUBLANES)
            piece = {}
            for i, j in INDEX:
                mine = mine_ref[i, j, rows, lanes]
                other = other_ref[i, j, rows, lanes]
                piece[i, j] = (
                    vis_ref[0, i, j, rows, lanes] - jnp.where(first, mine, other),
                    vis_ref[1, i, j, rows, lanes] - jnp.where(first, other, mine),
                )
            resid.append(piece)
        for k in range(dirs):
            jones_p = read_rows(gathered_ref, dirs, k, base, LANES)
            jones_q = read_rows(gathered_ref, dirs, k, baselines + base, LANES)
            sums = None
            for index, time in enumerate(range(0, times, SUBLANES)):
                rows = slice(time, time + SUBLANES)
                coher = {(i, j): tuple(coher_ref[k, part, i, j, rows, lanes] for part in range(2)) for i, j in INDEX}
                along = mat_mul_h(coher, jones_q)
                ahead = mat_mul(jones_p, coher)
                right_p = mat_mul_h(resid[index], along)
                right_q = mat_h_mul(resid[index], ahead)
                cross_p = cadd(cmul_conj(along[0, 0], along[1, 0]), cmul_conj(along[0, 1], along[1, 1]))
                cross_q = cadd(cmul_conj(ahead[0, 1], ahead[0, 0]), cmul_conj(ahead[1, 1], ahead[1, 0]))
                terms_p = [right_p[ij][part] for part in range(2) for ij in INDEX] + [
                    sq(along[0, 0]) + sq(along[0, 1]),
                    sq(along[1, 0]) + sq(along[1, 1]),
                    cross_p[0],
                    cross_p[1],
                ]
                terms_q = [right_q[ij][part] for part in range(2) for ij in INDEX] + [
                    sq(ahead[0, 0]) + sq(ahead[1, 0]),
                    sq(ahead[0, 1]) + sq(ahead[1, 1]),
                    cross_q[0],
                    cross_q[1],
                ]
                terms = terms_p + terms_q
                sums = terms if sums is None else [a + b for a, b in zip(sums, terms)]
            for at, term in enumerate(sums):
                row = (at % 12) * dirs + k
                offset = base + (at // 12) * baselines
                left_ref[row : row + 1, offset : offset + LANES] = jnp.sum(term, axis=0, keepdims=True)

    def group(ref, at):
        return ref[at * dirs : (at + 1) * dirs, :]

    jones = {(i, j): (group(gathered_ref, comp(0, i, j)), group(gathered_ref, comp(1, i, j))) for i, j in INDEX}
    diag0, diag1 = group(left_ref, 8), group(left_ref, 9)
    off = (group(left_ref, 10), group(left_ref, 11))
    off_c = (off[0], -off[1])
    for i in range(2):
        left, right = jones[i, 0], jones[i, 1]
        col0 = cadd((left[0] * diag0, left[1] * diag0), cmul(right, off_c))
        col1 = cadd(cmul(left, off), (right[0] * diag1, right[1] * diag1))
        for j, col in ((0, col0), (1, col1)):
            for part in range(2):
                at = comp(part, i, j) * dirs
                left_ref[at : at + dirs, :] = left_ref[at : at + dirs, :] + col[part]

    sums = split_dot(left_ref[...], onehot_ref[...], ((1,), (1,)))
    store_chunks(sums_ref, 0, sums[: 8 * dirs])
    m00 = sums[8 * dirs : 9 * dirs] + RHO
    m11 = sums[9 * dirs : 10 * dirs] + RHO
    m01 = (sums[10 * dirs : 11 * dirs], sums[11 * dirs : 12 * dirs])
    scale = 1.0 / (m00 * m11 - sq(m01))
    store_chunks(sums_ref, 8 * dirs, m11 * scale)
    store_chunks(sums_ref, 9 * dirs, m00 * scale)
    store_chunks(sums_ref, 10 * dirs, -m01[0] * scale)
    store_chunks(sums_ref, 11 * dirs, -m01[1] * scale)


def solve(sums, known, dirs):
    i00, i11, re01, im01 = (sums(at * dirs) for at in range(8, 12))
    i01, i10 = (re01, im01), (re01, -im01)
    out = {}
    for i in range(2):
        n = []
        for j in range(2):
            at = [comp(part, i, j) * dirs for part in range(2)]
            n.append(tuple(sums(a) + known(a) for a in at))
        left = cadd((n[0][0] * i00, n[0][1] * i00), cmul(n[1], i10))
        right = cadd(cmul(n[0], i01), (n[1][0] * i11, n[1][1] * i11))
        for part in range(2):
            out[comp(part, i, 0) * dirs] = left[part]
            out[comp(part, i, 1) * dirs] = right[part]
    return out


def first_update_kernel(basis_ref, sums_ref, known_ref, lag_ref, jones_ref, unit_ref):
    dirs = sums_ref.shape[1] // 12
    chunks, rows, width = known_ref.shape
    terms = basis_ref.shape[1]
    for chunk in range(chunks):
        out = solve(
            lambda a: sums_ref[chunk, a : a + dirs, :], lambda a: known_ref[chunk, a : a + dirs, :], dirs
        )
        for a, value in out.items():
            jones_ref[a : a + dirs, chunk * width : (chunk + 1) * width] = value
            at = chunk * rows + a
            unit_ref[at : at + dirs, :] = value + lag_ref[chunk, a : a + dirs, :]
    unit_ref[chunks * rows :, :] = jnp.zeros((SUBLANES, width), jnp.float32)
    unit_ref[chunks * rows : chunks * rows + 1, :terms] = basis_ref[...]


def solve_next(sums, consensus, before, dirs):
    out = solve(sums, lambda a: RHO * (2.0 * consensus(a) - before(a)), dirs)
    return out, {a: value + (before(a) - consensus(a)) for a, value in out.items()}


def solve_chunk(chunk, sums_ref, consensus_ref, before_ref):
    dirs = sums_ref.shape[1] // 12

    def rows(ref):
        return lambda a: ref[chunk, a : a + dirs, :]

    return solve_next(rows(sums_ref), rows(consensus_ref), rows(before_ref), dirs)


def update_kernel(sums_ref, consensus_ref, before_ref, jones_ref, shared_ref):
    dirs, width = sums_ref.shape[1] // 12, sums_ref.shape[2]
    for chunk in range(sums_ref.shape[0]):
        jones, shared = solve_chunk(chunk, sums_ref, consensus_ref, before_ref)
        for a in jones:
            jones_ref[a : a + dirs, chunk * width : (chunk + 1) * width] = jones[a]
            shared_ref[chunk, a : a + dirs, :] = shared[a]


def store_native(chunk, width, dirs, rows, ref):
    for part in range(2):
        for i, j in INDEX:
            value = rows[comp(part, i, j) * dirs]
            for k in range(dirs):
                ref[k, part, i, j : j + 1, chunk * width : (chunk + 1) * width] = value[k : k + 1, :]


def last_update_kernel(sums_ref, consensus_ref, before_ref, jones_ref, shared_ref):
    dirs, width = sums_ref.shape[1] // 12, sums_ref.shape[2]
    for chunk in range(sums_ref.shape[0]):
        jones, shared = solve_chunk(chunk, sums_ref, consensus_ref, before_ref)
        store_native(chunk, width, dirs, jones, jones_ref)
        store_native(chunk, width, dirs, shared, shared_ref)


def weighted(matrix, g, values):
    total = None
    for f, value in enumerate(values):
        weight = jnp.broadcast_to(matrix[g : g + 1, f : f + 1], value.shape[-2:])
        total = weight * value if total is None else total + weight * value
    return total


def gathered_update_kernel(sums_ref, *refs):
    units, (jones_ref, shared_ref, spread_ref, weights_ref) = refs[:-4], refs[-4:]
    own, tail = units[0], units[-1]
    dirs = sums_ref.shape[1] // 12
    chunks, _, width = sums_ref.shape
    rows = 8 * dirs
    terms = weights_ref.shape[0]
    bands = len(units) - 1
    hi = lax.Precision.HIGHEST
    at = chunks * rows
    start = own.shape[0] - tail.shape[0]
    basis = jnp.concatenate(
        [ref[at : at + 1, :terms] for ref in units[:-2]] + [tail[at - start : at - start + 1, :terms]], axis=0
    )
    gram = lax.dot_general(basis, basis, (((0,), (0,)), ((), ())), precision=hi, preferred_element_type=jnp.float32)
    row = lax.broadcasted_iota(jnp.int32, (terms, terms), 0)
    col = lax.broadcasted_iota(jnp.int32, (terms, terms), 1)
    gram = gram + jnp.where(row == col, RIDGE * bands, 0.0)
    inverse = jnp.where(row == col, 1.0, 0.0)
    for t in range(terms):
        scale = 1.0 / gram[t : t + 1, t : t + 1]
        g_row = gram[t : t + 1, :] * scale
        i_row = inverse[t : t + 1, :] * scale
        factor = gram[:, t : t + 1]
        here = row == t
        gram = jnp.where(here, g_row, gram - factor * g_row)
        inverse = jnp.where(here, i_row, inverse - factor * i_row)
    weights = lax.dot_general(inverse, basis, (((1,), (1,)), ((), ())), precision=hi, preferred_element_type=jnp.float32)
    spread = jnp.dot(basis, weights, precision=hi, preferred_element_type=jnp.float32)
    spread_ref[...] = spread
    weights_ref[...] = weights
    for chunk in range(chunks):
        jones, shared = solve_gathered(chunk, spread, sums_ref, units, rows)
        for a in jones:
            jones_ref[a : a + dirs, chunk * width : (chunk + 1) * width] = jones[a]
            shared_ref[chunk * rows + a : chunk * rows + a + dirs, :] = shared[a]


def solve_gathered(chunk, spread, sums_ref, units, rows):
    dirs = sums_ref.shape[1] // 12
    head, tail = units[-2:]
    base, start = chunk * rows, head.shape[0]
    values = [ref[base : base + rows, :] for ref in units[:-2]]
    values.append(head[base : base + rows, :] if base < start else tail[base - start : base - start + rows, :])
    consensus = weighted(spread, 0, values)
    return solve_next(
        lambda a: sums_ref[chunk, a : a + dirs, :],
        lambda a: consensus[a : a + dirs],
        lambda a: values[0][a : a + dirs],
        dirs,
    )


def partial_consensus_kernel(spread_ref, *refs):
    units, out_ref = refs[:-1], refs[-1]
    rows = out_ref.shape[0]
    spread = spread_ref[...]
    step = 4 * SUBLANES
    for base in range(0, rows, step):
        out_ref[base : base + step, :] = weighted(spread, 0, [ref[base : base + step, :] for ref in units])


def gathered_last_kernel(spread_ref, sums_ref, own_ref, partial_ref, head_ref, tail_ref, jones_ref, shared_ref):
    dirs, width = sums_ref.shape[1] // 12, sums_ref.shape[2]
    rows = 8 * dirs
    bands = spread_ref.shape[0]
    start = head_ref.shape[0]
    last = spread_ref[0:1, bands - 1 : bands]
    for chunk in range(sums_ref.shape[0]):
        base = chunk * rows
        far = head_ref[base : base + rows, :] if base < start else tail_ref[base - start : base - start + rows, :]
        consensus = partial_ref[base : base + rows, :] + jnp.broadcast_to(last, far.shape) * far
        jones, shared = solve_next(
            lambda a: sums_ref[chunk, a : a + dirs, :],
            lambda a: consensus[a : a + dirs],
            lambda a: own_ref[base + a : base + a + dirs, :],
            dirs,
        )
        for a in jones:
            jones_ref[a : a + dirs, chunk * width : (chunk + 1) * width] = jones[a]
        store_native(chunk, width, dirs, shared, shared_ref)


def native_kernel(rows_ref, out_ref):
    dirs = out_ref.shape[0]
    rows = {a: rows_ref[a : a + dirs, :] for a in range(0, 8 * dirs, dirs)}
    store_native(0, rows_ref.shape[1], dirs, rows, out_ref)


def partial_coeffs_kernel(weights_ref, *refs):
    units, out_ref = refs[:-1], refs[-1]
    weights = weights_ref[...]
    for k in range(out_ref.shape[1]):
        for part in range(2):
            for i in range(2):
                values = [ref[k, part, i] for ref in units]
                for m in range(weights.shape[0]):
                    out_ref[m, k, part, i] = weighted(weights, m, values)


def final_kernel(
    basis_ref, weights_ref, own_ref, partial_ref, head_ref, tail_ref, coeffs_hbm, dual_hbm, coeffs_ref, dual_ref, sems
):
    terms, dirs = coeffs_ref.shape[:2]
    half = head_ref.shape[0]
    weights = weights_ref[...]
    far = weights.shape[1] - 1
    copies = []
    for k in range(dirs):
        for part in range(2):
            for i in range(2):
                value = head_ref[k, part, i] if k < half else tail_ref[k - half, part, i]
                consensus = None
                for m in range(terms):
                    weight = jnp.broadcast_to(weights[m : m + 1, far:], value.shape)
                    total = partial_ref[m, k, part, i] + weight * value
                    coeffs_ref[m, k, part, i] = total
                    share = total * basis_ref[0, m]
                    consensus = share if consensus is None else consensus + share
                dual_ref[k, part, i] = RHO * (own_ref[k, part, i] - consensus)
        copies.append(pltpu.make_async_copy(coeffs_ref.at[:, k], coeffs_hbm.at[:, k], sems.at[k]))
        copies[-1].start()
    copies.append(pltpu.make_async_copy(dual_ref, dual_hbm, sems.at[dirs]))
    copies[-1].start()
    for copy in copies:
        copy.wait()


def struct(*shape, dtype=jnp.float32):
    return jax.ShapeDtypeStruct(shape, dtype)


def call(kernel, out_shape, scalars, args, scratch=(), space=VMEM, out_space=VMEM):
    many = isinstance(out_shape, (tuple, list))
    return pl.pallas_call(
        kernel,
        out_shape=out_shape,
        in_specs=[SMEM if at < scalars else space for at in range(len(args))],
        out_specs=tuple(out_space for _ in out_shape) if many else out_space,
        scratch_shapes=list(scratch),
        compiler_params=PARAMS,
    )(*args)


def swap(value, axis, bit):
    size = lax.axis_size(axis)
    return lax.ppermute(value, axis, [(i, i ^ bit) for i in range(size)])


def sum_over_dir(mine, other):
    size = lax.axis_size("dir")
    mine = mine + swap(other, "dir", 1)
    bit = 2
    while bit < size:
        mine = mine + swap(mine, "dir", bit)
        bit *= 2
    return mine, swap(mine, "dir", 1)


def ring_gather(value, half):
    size = lax.axis_size("band")
    order = list(range(0, size, 2)) + list(range(size - 1, 0, -2))
    ahead = [(order[i], order[(i + 1) % size]) for i in range(size)]
    behind = [(b, a) for a, b in ahead]
    values = [value]
    up = down = value
    for step in range(1, (size - 1) // 2 + 1):
        up = lax.ppermute(up, "band", ahead)
        down = lax.ppermute(down, "band", behind)
        values += [up, down]
    return values + [lax.ppermute(up[:half], "band", ahead), lax.ppermute(down[half:], "band", behind)]


def reduce_bands(shared, row, factor):
    sums = lax.psum(row.reshape((-1,) + (1,) * shared.ndim) * shared[None], "band")
    flat = sums.reshape(sums.shape[0], -1)
    return jax.scipy.linalg.cho_solve((factor, True), flat).reshape(sums.shape)


def local(visibilities, coherencies, jones_start, dual_start, consensus_start, freq_basis, pairs):
    row = freq_basis[0]
    terms = row.shape[0]
    bands = lax.axis_size("band")
    vis, coher = visibilities[0], coherencies[0]
    native = jones_start.shape[1:]
    dirs, stations = native[0], native[-1]
    times, baselines = coher.shape[-2:]
    rows = 8 * dirs
    parity = (lax.axis_index("dir") % 2).astype(jnp.int32).reshape(1, 1)
    chunked = stations % (bands * LANES) == 0 and bands % 2 == 0 and dirs % 2 == 0
    hi = lax.Precision.HIGHEST
    width = stations // bands if chunked else LANES
    chunks = stations // width
    half = struct(2, 2, times, baselines)
    flat = struct(rows, stations)
    spread_rows = struct(chunks, rows, width)
    onehot = pltpu.VMEM((stations, 2 * baselines), jnp.bfloat16)
    left = pltpu.VMEM((12 * dirs, 2 * baselines), jnp.float32)
    model_out = (struct(rows, 2 * baselines), half, half)

    if not chunked:
        gram = lax.psum(row[:, None] * row[None, :], "band") + RIDGE * bands * jnp.eye(terms, dtype=jnp.float32)
        factor = jnp.linalg.cholesky(gram)

    def model(jones):
        return call(model_kernel, model_out, 1, (parity, jones, pairs, coher), [onehot])

    def station_sums(gathered, mine, other):
        mine, other = sum_over_dir(mine, other)
        return call(
            sums_kernel, struct(chunks, 12 * dirs, width), 1,
            (parity, gathered, pairs, coher, vis, mine, other), [onehot, left],
        )

    def share(shared):
        coeffs = reduce_bands(shared, row, factor)
        return coeffs, jnp.tensordot(row, coeffs, axes=(0, 0), precision=hi)

    started = call(
        first_model_kernel, model_out, 1,
        (parity, *(pltpu.with_memory_space_constraint(x, pltpu.HBM) for x in (jones_start[0], pairs, coher))),
        [
            onehot,
            pltpu.VMEM((rows, stations), jnp.float32),
            pltpu.VMEM(native, jnp.float32),
            pltpu.VMEM(pairs.shape, pairs.dtype),
            pltpu.VMEM(coher.shape, jnp.float32),
            pltpu.SemaphoreType.DMA((3,)),
        ],
        HBM,
    )
    known, lag = call(prepare_kernel, (spread_rows,) * 2, 1, (freq_basis, dual_start[0], consensus_start))
    jones, unit = call(
        first_update_kernel, (flat, struct(stations * rows // width + SUBLANES, width)), 0,
        (freq_basis, station_sums(*started), known, lag),
    )
    if chunked:
        half_rows = chunks // 2 * rows
        units = ring_gather(unit, half_rows)
        sums = station_sums(*model(jones))
        jones, unit, spread, weights = call(
            gathered_update_kernel,
            (flat, struct(chunks * rows, width), struct(bands, bands), struct(terms, bands)), 0, (sums, *units),
        )
        units = ring_gather(unit, half_rows)
        sums = station_sums(*model(jones))
        partial = call(partial_consensus_kernel, struct(chunks * rows, width), 0, (spread, *units[:-2]))
        jones, shared = call(
            gathered_last_kernel, (flat, struct(*native)), 0, (spread, sums, unit, partial, *units[-2:])
        )
        jones = call(native_kernel, struct(*native), 0, (jones,))
        units = ring_gather(shared, dirs // 2)
        partial = call(partial_coeffs_kernel, struct(terms, *native), 0, (weights, *units[:-2]))
        coeffs, dual = call(
            final_kernel, (struct(terms, *native), struct(*native)), 1,
            (freq_basis, weights, shared, partial, *units[-2:]),
            [
                pltpu.VMEM((terms, *native), jnp.float32),
                pltpu.VMEM(native, jnp.float32),
                pltpu.SemaphoreType.DMA((dirs + 1,)),
            ],
            out_space=HBM,
        )
    else:
        shared = unit[: chunks * rows].reshape(spread_rows.shape)
        for _ in range(ITERS - 2):
            consensus = share(shared)[1]
            sums = station_sums(*model(jones))
            jones, shared = call(update_kernel, (flat, spread_rows), 0, (sums, consensus, shared))
        consensus = share(shared)[1]
        sums = station_sums(*model(jones))
        jones, shared = call(last_update_kernel, (struct(*native),) * 2, 0, (sums, consensus, shared))
        coeffs, consensus = share(shared)
        dual = RHO * (shared - consensus)
    return jones[None], dual[None], coeffs


def solution(mesh):
    in_specs = (
        P("band", None, None, None, None, None),
        P("band", "dir", None, None, None, None, None),
        P("band", "dir", None, None, None, None),
        P("band", "dir", None, None, None, None),
        P(None, "dir", None, None, None, None),
        P("band", None),
        P(),
    )
    out_specs = (
        P("band", "dir", None, None, None, None),
        P("band", "dir", None, None, None, None),
        P(None, "dir", None, None, None, None),
    )
    return jax.shard_map(local, mesh=mesh, in_specs=in_specs, out_specs=out_specs, check_vma=False)
```

```python
import jax
import jax.numpy as jnp
from jax import lax
from jax.experimental import pallas as pl
from jax.experimental.pallas import tpu as pltpu
from jax.sharding import PartitionSpec as P

ITERS = 3
RHO = 5.0
RIDGE = 0.25
LANES = 128
SUBLANES = 8

VMEM = pl.BlockSpec(memory_space=pltpu.VMEM)
SMEM = pl.BlockSpec(memory_space=pltpu.SMEM)
HBM = pl.BlockSpec(memory_space=pltpu.HBM)
PARAMS = pltpu.CompilerParams(vmem_limit_bytes=16 * 1024 * 1024)

INDEX = ((0, 0), (0, 1), (1, 0), (1, 1))


def comp(part, i, j):
    return part * 4 + i * 2 + j


def cadd(a, b):
    return (a[0] + b[0], a[1] + b[1])


def cmul(a, b):
    return (a[0] * b[0] - a[1] * b[1], a[0] * b[1] + a[1] * b[0])


def cmul_conj(a, b):
    return (a[0] * b[0] + a[1] * b[1], a[1] * b[0] - a[0] * b[1])


def mat_mul(a, b):
    return {(i, j): cadd(cmul(a[i, 0], b[0, j]), cmul(a[i, 1], b[1, j])) for i, j in INDEX}


def mat_mul_h(a, b):
    return {(i, j): cadd(cmul_conj(a[i, 0], b[j, 0]), cmul_conj(a[i, 1], b[j, 1])) for i, j in INDEX}


def mat_h_mul(a, b):
    return {(i, j): cadd(cmul_conj(b[0, j], a[0, i]), cmul_conj(b[1, j], a[1, i])) for i, j in INDEX}


def sq(a):
    return a[0] * a[0] + a[1] * a[1]


def split_dot(left, right, dims):
    high = left.astype(jnp.bfloat16)
    low = (left - high.astype(jnp.float32)).astype(jnp.bfloat16)
    both = jnp.concatenate([high, low], axis=0)
    out = lax.dot_general(both, right, (dims, ((), ())), preferred_element_type=jnp.float32)
    return out[: left.shape[0]] + out[left.shape[0] :]


def fill_onehot(pairs_ref, onehot_ref):
    stations = onehot_ref.shape[0]
    baselines = pairs_ref.shape[1]
    for half in range(2):
        ids = pairs_ref[half : half + 1, :]
        for base in range(0, stations, LANES):
            station = lax.broadcasted_iota(jnp.int32, (LANES, baselines), 0) + base
            hit = jnp.where(station == ids, 1.0, 0.0).astype(jnp.bfloat16)
            onehot_ref[base : base + LANES, half * baselines : (half + 1) * baselines] = hit


def read_rows(ref, dirs, k, base, width):
    def one(part, i, j):
        row = comp(part, i, j) * dirs + k
        return jnp.broadcast_to(ref[row : row + 1, base : base + width], (SUBLANES, width))

    return {(i, j): (one(0, i, j), one(1, i, j)) for i, j in INDEX}


def native_to_rows(block, dirs, store):
    for k in range(dirs):
        for part in range(2):
            for i in range(2):
                value = block(k, part, i)
                for j in range(2):
                    store(comp(part, i, j) * dirs + k, value[j : j + 1, :])


def store_chunks(ref, row, value):
    width = ref.shape[2]
    for chunk in range(ref.shape[0]):
        ref[chunk, row : row + value.shape[0], :] = value[:, chunk * width : (chunk + 1) * width]


def prepare_kernel(basis_ref, dual_ref, coeffs_ref, known_ref, lag_ref):
    terms, dirs = coeffs_ref.shape[:2]

    def known(k, part, i):
        total = coeffs_ref[0, k, part, i] * basis_ref[0, 0]
        for m in range(1, terms):
            total = total + coeffs_ref[m, k, part, i] * basis_ref[0, m]
        return RHO * total - dual_ref[k, part, i]

    native_to_rows(known, dirs, lambda row, value: store_chunks(known_ref, row, value))
    native_to_rows(
        lambda k, part, i: dual_ref[k, part, i] * (1.0 / RHO), dirs,
        lambda row, value: store_chunks(lag_ref, row, value),
    )


def model_body(parity_ref, jones, onehot_ref, coher_ref, gathered_ref, mine_ref, other_ref):
    dirs = coher_ref.shape[0]
    times, baselines = coher_ref.shape[-2:]
    gathered_ref[...] = split_dot(jones, onehot_ref[...], ((1,), (0,)))
    first = parity_ref[0, 0] == 0
    for base in range(0, baselines, LANES):
        lanes = slice(base, base + LANES)
        for time in range(0, times, SUBLANES):
            rows = slice(time, time + SUBLANES)
            total = None
            for k in range(dirs):
                jones_p = read_rows(gathered_ref, dirs, k, base, LANES)
                jones_q = read_rows(gathered_ref, dirs, k, baselines + base, LANES)
                coher = {(i, j): tuple(coher_ref[k, part, i, j, rows, lanes] for part in range(2)) for i, j in INDEX}
                model = mat_mul(jones_p, mat_mul_h(coher, jones_q))
                total = model if total is None else {ij: cadd(total[ij], model[ij]) for ij in INDEX}
            for i, j in INDEX:
                real, imag = total[i, j]
                mine_ref[i, j, rows, lanes] = jnp.where(first, real, imag)
                other_ref[i, j, rows, lanes] = jnp.where(first, imag, real)


def first_model_kernel(
    parity_ref, jones_hbm, pairs_hbm, coher_hbm, gathered_ref, mine_ref, other_ref,
    onehot_ref, rows_ref, jones_ref, pairs_ref, coher_ref, sems,
):
    copies = [
        pltpu.make_async_copy(source, target, sems.at[at])
        for at, (source, target) in enumerate(
            ((pairs_hbm, pairs_ref), (jones_hbm, jones_ref), (coher_hbm, coher_ref))
        )
    ]
    for copy in copies:
        copy.start()
    copies[0].wait()
    fill_onehot(pairs_ref, onehot_ref)
    copies[1].wait()

    def store(row, value):
        rows_ref[row : row + 1, :] = value

    native_to_rows(lambda k, part, i: jones_ref[k, part, i], coher_ref.shape[0], store)
    copies[2].wait()
    model_body(parity_ref, rows_ref[...], onehot_ref, coher_ref, gathered_ref, mine_ref, other_ref)


def model_kernel(parity_ref, jones_ref, pairs_ref, coher_ref, gathered_ref, mine_ref, other_ref, onehot_ref):
    fill_onehot(pairs_ref, onehot_ref)
    model_body(parity_ref, jones_ref[...], onehot_ref, coher_ref, gathered_ref, mine_ref, other_ref)


def sums_kernel(
    parity_ref, gathered_ref, pairs_ref, coher_ref, vis_ref, mine_ref, other_ref, sums_ref, onehot_ref, left_ref
):
    dirs = coher_ref.shape[0]
    times, baselines = coher_ref.shape[-2:]
    fill_onehot(pairs_ref, onehot_ref)
    first = parity_ref[0, 0] == 0
    for base in range(0, baselines, LANES):
        lanes = slice(base, base + LANES)
        resid = []
        for time in range(0, times, SUBLANES):
            rows = slice(time, time + SUBLANES)
            piece = {}
            for i, j in INDEX:
                mine = mine_ref[i, j, rows, lanes]
                other = other_ref[i, j, rows, lanes]
                piece[i, j] = (
                    vis_ref[0, i, j, rows, lanes] - jnp.where(first, mine, other),
                    vis_ref[1, i, j, rows, lanes] - jnp.where(first, other, mine),
                )
            resid.append(piece)
        for k in range(dirs):
            jones_p = read_rows(gathered_ref, dirs, k, base, LANES)
            jones_q = read_rows(gathered_ref, dirs, k, baselines + base, LANES)
            sums = None
            for index, time in enumerate(range(0, times, SUBLANES)):
                rows = slice(time, time + SUBLANES)
                coher = {(i, j): tuple(coher_ref[k, part, i, j, rows, lanes] for part in range(2)) for i, j in INDEX}
                along = mat_mul_h(coher, jones_q)
                ahead = mat_mul(jones_p, coher)
                right_p = mat_mul_h(resid[index], along)
                right_q = mat_h_mul(resid[index], ahead)
                cross_p = cadd(cmul_conj(along[0, 0], along[1, 0]), cmul_conj(along[0, 1], along[1, 1]))
                cross_q = cadd(cmul_conj(ahead[0, 1], ahead[0, 0]), cmul_conj(ahead[1, 1], ahead[1, 0]))
                terms_p = [right_p[ij][part] for part in range(2) for ij in INDEX] + [
                    sq(along[0, 0]) + sq(along[0, 1]),
                    sq(along[1, 0]) + sq(along[1, 1]),
                    cross_p[0],
                    cross_p[1],
                ]
                terms_q = [right_q[ij][part] for part in range(2) for ij in INDEX] + [
                    sq(ahead[0, 0]) + sq(ahead[1, 0]),
                    sq(ahead[0, 1]) + sq(ahead[1, 1]),
                    cross_q[0],
                    cross_q[1],
                ]
                terms = terms_p + terms_q
                sums = terms if sums is None else [a + b for a, b in zip(sums, terms)]
            for at, term in enumerate(sums):
                row = (at % 12) * dirs + k
                offset = base + (at // 12) * baselines
                left_ref[row : row + 1, offset : offset + LANES] = jnp.sum(term, axis=0, keepdims=True)

    def group(ref, at):
        return ref[at * dirs : (at + 1) * dirs, :]

    jones = {(i, j): (group(gathered_ref, comp(0, i, j)), group(gathered_ref, comp(1, i, j))) for i, j in INDEX}
    diag0, diag1 = group(left_ref, 8), group(left_ref, 9)
    off = (group(left_ref, 10), group(left_ref, 11))
    off_c = (off[0], -off[1])
    for i in range(2):
        left, right = jones[i, 0], jones[i, 1]
        col0 = cadd((left[0] * diag0, left[1] * diag0), cmul(right, off_c))
        col1 = cadd(cmul(left, off), (right[0] * diag1, right[1] * diag1))
        for j, col in ((0, col0), (1, col1)):
            for part in range(2):
                at = comp(part, i, j) * dirs
                left_ref[at : at + dirs, :] = left_ref[at : at + dirs, :] + col[part]

    sums = split_dot(left_ref[...], onehot_ref[...], ((1,), (1,)))
    store_chunks(sums_ref, 0, sums[: 8 * dirs])
    m00 = sums[8 * dirs : 9 * dirs] + RHO
    m11 = sums[9 * dirs : 10 * dirs] + RHO
    m01 = (sums[10 * dirs : 11 * dirs], sums[11 * dirs : 12 * dirs])
    scale = 1.0 / (m00 * m11 - sq(m01))
    store_chunks(sums_ref, 8 * dirs, m11 * scale)
    store_chunks(sums_ref, 9 * dirs, m00 * scale)
    store_chunks(sums_ref, 10 * dirs, -m01[0] * scale)
    store_chunks(sums_ref, 11 * dirs, -m01[1] * scale)


def solve(sums, known, dirs):
    i00, i11, re01, im01 = (sums(at * dirs) for at in range(8, 12))
    i01, i10 = (re01, im01), (re01, -im01)
    out = {}
    for i in range(2):
        n = []
        for j in range(2):
            at = [comp(part, i, j) * dirs for part in range(2)]
            n.append(tuple(sums(a) + known(a) for a in at))
        left = cadd((n[0][0] * i00, n[0][1] * i00), cmul(n[1], i10))
        right = cadd(cmul(n[0], i01), (n[1][0] * i11, n[1][1] * i11))
        for part in range(2):
            out[comp(part, i, 0) * dirs] = left[part]
            out[comp(part, i, 1) * dirs] = right[part]
    return out


def first_update_kernel(basis_ref, sums_ref, known_ref, lag_ref, jones_ref, unit_ref):
    dirs = sums_ref.shape[1] // 12
    chunks, rows, width = known_ref.shape
    terms = basis_ref.shape[1]
    for chunk in range(chunks):
        out = solve(
            lambda a: sums_ref[chunk, a : a + dirs, :], lambda a: known_ref[chunk, a : a + dirs, :], dirs
        )
        for a, value in out.items():
            jones_ref[a : a + dirs, chunk * width : (chunk + 1) * width] = value
            at = chunk * rows + a
            unit_ref[at : at + dirs, :] = value + lag_ref[chunk, a : a + dirs, :]
    unit_ref[chunks * rows :, :] = jnp.zeros((SUBLANES, width), jnp.float32)
    unit_ref[chunks * rows : chunks * rows + 1, :terms] = basis_ref[...]


def solve_next(sums, consensus, before, dirs):
    out = solve(sums, lambda a: RHO * (2.0 * consensus(a) - before(a)), dirs)
    return out, {a: value + (before(a) - consensus(a)) for a, value in out.items()}


def solve_chunk(chunk, sums_ref, consensus_ref, before_ref):
    dirs = sums_ref.shape[1] // 12

    def rows(ref):
        return lambda a: ref[chunk, a : a + dirs, :]

    return solve_next(rows(sums_ref), rows(consensus_ref), rows(before_ref), dirs)


def update_kernel(sums_ref, consensus_ref, before_ref, jones_ref, shared_ref):
    dirs, width = sums_ref.shape[1] // 12, sums_ref.shape[2]
    for chunk in range(sums_ref.shape[0]):
        jones, shared = solve_chunk(chunk, sums_ref, consensus_ref, before_ref)
        for a in jones:
            jones_ref[a : a + dirs, chunk * width : (chunk + 1) * width] = jones[a]
            shared_ref[chunk, a : a + dirs, :] = shared[a]


def store_native(chunk, width, dirs, rows, ref):
    for part in range(2):
        for i, j in INDEX:
            value = rows[comp(part, i, j) * dirs]
            for k in range(dirs):
                ref[k, part, i, j : j + 1, chunk * width : (chunk + 1) * width] = value[k : k + 1, :]


def last_update_kernel(sums_ref, consensus_ref, before_ref, jones_ref, shared_ref):
    dirs, width = sums_ref.shape[1] // 12, sums_ref.shape[2]
    for chunk in range(sums_ref.shape[0]):
        jones, shared = solve_chunk(chunk, sums_ref, consensus_ref, before_ref)
        store_native(chunk, width, dirs, jones, jones_ref)
        store_native(chunk, width, dirs, shared, shared_ref)


def weighted(matrix, g, values):
    total = None
    for f, value in enumerate(values):
        weight = jnp.broadcast_to(matrix[g : g + 1, f : f + 1], value.shape[-2:])
        total = weight * value if total is None else total + weight * value
    return total


def gathered_update_kernel(sums_ref, *refs):
    units, (jones_ref, shared_ref, spread_ref, weights_ref) = refs[:-4], refs[-4:]
    dirs = sums_ref.shape[1] // 12
    chunks, _, width = sums_ref.shape
    rows = 8 * dirs
    terms = weights_ref.shape[0]
    bands = len(units)
    hi = lax.Precision.HIGHEST
    at = chunks * rows
    basis = jnp.concatenate([ref[at : at + 1, :terms] for ref in units], axis=0)
    gram = lax.dot_general(basis, basis, (((0,), (0,)), ((), ())), precision=hi, preferred_element_type=jnp.float32)
    row = lax.broadcasted_iota(jnp.int32, (terms, terms), 0)
    col = lax.broadcasted_iota(jnp.int32, (terms, terms), 1)
    gram = gram + jnp.where(row == col, RIDGE * bands, 0.0)
    inverse = jnp.where(row == col, 1.0, 0.0)
    for t in range(terms):
        scale = 1.0 / gram[t : t + 1, t : t + 1]
        g_row = gram[t : t + 1, :] * scale
        i_row = inverse[t : t + 1, :] * scale
        factor = gram[:, t : t + 1]
        here = row == t
        gram = jnp.where(here, g_row, gram - factor * g_row)
        inverse = jnp.where(here, i_row, inverse - factor * i_row)
    weights = lax.dot_general(inverse, basis, (((1,), (1,)), ((), ())), precision=hi, preferred_element_type=jnp.float32)
    spread = jnp.dot(basis, weights, precision=hi, preferred_element_type=jnp.float32)
    spread_ref[...] = spread
    weights_ref[...] = weights
    for chunk in range(chunks):
        jones, shared = solve_gathered(chunk, spread, sums_ref, units, rows)
        for a in jones:
            jones_ref[a : a + dirs, chunk * width : (chunk + 1) * width] = jones[a]
            shared_ref[chunk * rows + a : chunk * rows + a + dirs, :] = shared[a]


def solve_gathered(chunk, spread, sums_ref, units, rows):
    dirs = sums_ref.shape[1] // 12
    base = chunk * rows
    values = [ref[base : base + rows, :] for ref in units]
    consensus = weighted(spread, 0, values)
    return solve_next(
        lambda a: sums_ref[chunk, a : a + dirs, :],
        lambda a: consensus[a : a + dirs],
        lambda a: values[0][a : a + dirs],
        dirs,
    )


def partial_consensus_kernel(spread_ref, *refs):
    units, out_ref = refs[:-1], refs[-1]
    rows = out_ref.shape[0]
    spread = spread_ref[...]
    step = 4 * SUBLANES
    for base in range(0, rows, step):
        out_ref[base : base + step, :] = weighted(spread, 0, [ref[base : base + step, :] for ref in units])


def gathered_last_kernel(spread_ref, sums_ref, own_ref, partial_ref, *refs):
    units, (jones_ref, shared_ref) = refs[:-2], refs[-2:]
    dirs, width = sums_ref.shape[1] // 12, sums_ref.shape[2]
    rows = 8 * dirs
    spread = spread_ref[0:1, spread_ref.shape[0] - len(units) :]
    for chunk in range(sums_ref.shape[0]):
        base = chunk * rows
        rest = weighted(spread, 0, [ref[base : base + rows, :] for ref in units])
        consensus = partial_ref[base : base + rows, :] + rest
        jones, shared = solve_next(
            lambda a: sums_ref[chunk, a : a + dirs, :],
            lambda a: consensus[a : a + dirs],
            lambda a: own_ref[base + a : base + a + dirs, :],
            dirs,
        )
        for a in jones:
            jones_ref[a : a + dirs, chunk * width : (chunk + 1) * width] = jones[a]
        store_native(chunk, width, dirs, shared, shared_ref)


def native_kernel(rows_ref, out_ref):
    dirs = out_ref.shape[0]
    rows = {a: rows_ref[a : a + dirs, :] for a in range(0, 8 * dirs, dirs)}
    store_native(0, rows_ref.shape[1], dirs, rows, out_ref)


def partial_coeffs_kernel(weights_ref, *refs):
    units, out_ref = refs[:-1], refs[-1]
    weights = weights_ref[...]
    for k in range(out_ref.shape[1]):
        for part in range(2):
            for i in range(2):
                values = [ref[k, part, i] for ref in units]
                for m in range(weights.shape[0]):
                    out_ref[m, k, part, i] = weighted(weights, m, values)


def final_kernel(basis_ref, weights_ref, own_ref, partial_ref, *refs):
    units, (coeffs_hbm, dual_hbm, coeffs_ref, dual_ref, sems) = refs[:-5], refs[-5:]
    terms, dirs = coeffs_ref.shape[:2]
    weights = weights_ref[:, weights_ref.shape[1] - len(units) :]
    copies = []
    for k in range(dirs):
        for part in range(2):
            for i in range(2):
                values = [ref[k, part, i] for ref in units]
                consensus = None
                for m in range(terms):
                    total = partial_ref[m, k, part, i] + weighted(weights, m, values)
                    coeffs_ref[m, k, part, i] = total
                    share = total * basis_ref[0, m]
                    consensus = share if consensus is None else consensus + share
                dual_ref[k, part, i] = RHO * (own_ref[k, part, i] - consensus)
        copies.append(pltpu.make_async_copy(coeffs_ref.at[:, k], coeffs_hbm.at[:, k], sems.at[k]))
        copies[-1].start()
    copies.append(pltpu.make_async_copy(dual_ref, dual_hbm, sems.at[dirs]))
    copies[-1].start()
    for copy in copies:
        copy.wait()


def struct(*shape, dtype=jnp.float32):
    return jax.ShapeDtypeStruct(shape, dtype)


def call(kernel, out_shape, scalars, args, scratch=(), space=VMEM, out_space=VMEM):
    many = isinstance(out_shape, (tuple, list))
    return pl.pallas_call(
        kernel,
        out_shape=out_shape,
        in_specs=[SMEM if at < scalars else space for at in range(len(args))],
        out_specs=tuple(out_space for _ in out_shape) if many else out_space,
        scratch_shapes=list(scratch),
        compiler_params=PARAMS,
    )(*args)


def swap(value, axis, bit):
    size = lax.axis_size(axis)
    return lax.ppermute(value, axis, [(i, i ^ bit) for i in range(size)])


def sum_over_dir(mine, other):
    size = lax.axis_size("dir")
    mine = mine + swap(other, "dir", 1)
    bit = 2
    while bit < size:
        mine = mine + swap(mine, "dir", bit)
        bit *= 2
    return mine, swap(mine, "dir", 1)


def gather_bands(value):
    half = lax.axis_size("band") // 2
    far = swap(value, "band", half)
    near = [value]
    for bit in range(1, half):
        near.append(swap(value, "band", bit))
    passed = [far]
    for bit in range(1, half):
        passed.append(swap(far, "band", bit))
    return near + passed


def reduce_bands(shared, row, factor):
    sums = lax.psum(row.reshape((-1,) + (1,) * shared.ndim) * shared[None], "band")
    flat = sums.reshape(sums.shape[0], -1)
    return jax.scipy.linalg.cho_solve((factor, True), flat).reshape(sums.shape)


def local(visibilities, coherencies, jones_start, dual_start, consensus_start, freq_basis, pairs):
    row = freq_basis[0]
    terms = row.shape[0]
    bands = lax.axis_size("band")
    vis, coher = visibilities[0], coherencies[0]
    native = jones_start.shape[1:]
    dirs, stations = native[0], native[-1]
    times, baselines = coher.shape[-2:]
    rows = 8 * dirs
    parity = (lax.axis_index("dir") % 2).astype(jnp.int32).reshape(1, 1)
    chunked = stations % (bands * LANES) == 0 and bands > 2 and bands & (bands - 1) == 0
    hi = lax.Precision.HIGHEST
    width = stations // bands if chunked else LANES
    chunks = stations // width
    half = struct(2, 2, times, baselines)
    flat = struct(rows, stations)
    spread_rows = struct(chunks, rows, width)
    onehot = pltpu.VMEM((stations, 2 * baselines), jnp.bfloat16)
    left = pltpu.VMEM((12 * dirs, 2 * baselines), jnp.float32)
    model_out = (struct(rows, 2 * baselines), half, half)

    if not chunked:
        gram = lax.psum(row[:, None] * row[None, :], "band") + RIDGE * bands * jnp.eye(terms, dtype=jnp.float32)
        factor = jnp.linalg.cholesky(gram)

    def model(jones):
        return call(model_kernel, model_out, 1, (parity, jones, pairs, coher), [onehot])

    def station_sums(gathered, mine, other):
        mine, other = sum_over_dir(mine, other)
        return call(
            sums_kernel, struct(chunks, 12 * dirs, width), 1,
            (parity, gathered, pairs, coher, vis, mine, other), [onehot, left],
        )

    def share(shared):
        coeffs = reduce_bands(shared, row, factor)
        return coeffs, jnp.tensordot(row, coeffs, axes=(0, 0), precision=hi)

    started = call(
        first_model_kernel, model_out, 1,
        (parity, *(pltpu.with_memory_space_constraint(x, pltpu.HBM) for x in (jones_start[0], pairs, coher))),
        [
            onehot,
            pltpu.VMEM((rows, stations), jnp.float32),
            pltpu.VMEM(native, jnp.float32),
            pltpu.VMEM(pairs.shape, pairs.dtype),
            pltpu.VMEM(coher.shape, jnp.float32),
            pltpu.SemaphoreType.DMA((3,)),
        ],
        HBM,
    )
    known, lag = call(prepare_kernel, (spread_rows,) * 2, 1, (freq_basis, dual_start[0], consensus_start))
    jones, unit = call(
        first_update_kernel, (flat, struct(stations * rows // width + SUBLANES, width)), 0,
        (freq_basis, station_sums(*started), known, lag),
    )
    if chunked:
        early = bands // 2 + 1
        units = gather_bands(unit)
        started = model(jones)
        sums = station_sums(*started)
        jones, unit, spread, weights = call(
            gathered_update_kernel,
            (flat, struct(chunks * rows, width), struct(bands, bands), struct(terms, bands)), 0, (sums, *units),
        )
        units = gather_bands(unit)
        started = model(jones)
        sums = station_sums(*started)
        partial = call(partial_consensus_kernel, struct(chunks * rows, width), 0, (spread, *units[:early]))
        jones, shared = call(
            gathered_last_kernel, (flat, struct(*native)), 0, (spread, sums, unit, partial, *units[early:])
        )
        jones = call(native_kernel, struct(*native), 0, (jones,))
        units = gather_bands(shared)
        partial = call(partial_coeffs_kernel, struct(terms, *native), 0, (weights, *units[:early]))
        coeffs, dual = call(
            final_kernel, (struct(terms, *native), struct(*native)), 1,
            (freq_basis, weights, shared, partial, *units[early:]),
            [
                pltpu.VMEM((terms, *native), jnp.float32),
                pltpu.VMEM(native, jnp.float32),
                pltpu.SemaphoreType.DMA((dirs + 1,)),
            ],
            out_space=HBM,
        )
    else:
        shared = unit[: chunks * rows].reshape(spread_rows.shape)
        for _ in range(ITERS - 2):
            consensus = share(shared)[1]
            sums = station_sums(*model(jones))
            jones, shared = call(update_kernel, (flat, spread_rows), 0, (sums, consensus, shared))
        consensus = share(shared)[1]
        sums = station_sums(*model(jones))
        jones, shared = call(last_update_kernel, (struct(*native),) * 2, 0, (sums, consensus, shared))
        coeffs, consensus = share(shared)
        dual = RHO * (shared - consensus)
    return jones[None], dual[None], coeffs


def solution(mesh):
    in_specs = (
        P("band", None, None, None, None, None),
        P("band", "dir", None, None, None, None, None),
        P("band", "dir", None, None, None, None),
        P("band", "dir", None, None, None, None),
        P(None, "dir", None, None, None, None),
        P("band", None),
        P(),
    )
    out_specs = (
        P("band", "dir", None, None, None, None),
        P("band", "dir", None, None, None, None),
        P(None, "dir", None, None, None, None),
    )

    return jax.shard_map(local, mesh=mesh, in_specs=in_specs, out_specs=out_specs, check_vma=False)
```

```python
import jax
import jax.numpy as jnp
from jax import lax
from jax.experimental import pallas as pl
from jax.experimental.pallas import tpu as pltpu
from jax.sharding import PartitionSpec as P

ITERS = 3
RHO = 5.0
RIDGE = 0.25
LANES = 128
SUBLANES = 8

VMEM = pl.BlockSpec(memory_space=pltpu.VMEM)
SMEM = pl.BlockSpec(memory_space=pltpu.SMEM)
HBM = pl.BlockSpec(memory_space=pltpu.HBM)
PARAMS = pltpu.CompilerParams(vmem_limit_bytes=16 * 1024 * 1024)

INDEX = ((0, 0), (0, 1), (1, 0), (1, 1))


def comp(part, i, j):
    return part * 4 + i * 2 + j


def cadd(a, b):
    return (a[0] + b[0], a[1] + b[1])


def cmul(a, b):
    return (a[0] * b[0] - a[1] * b[1], a[0] * b[1] + a[1] * b[0])


def cmul_conj(a, b):
    return (a[0] * b[0] + a[1] * b[1], a[1] * b[0] - a[0] * b[1])


def mat_mul(a, b):
    return {(i, j): cadd(cmul(a[i, 0], b[0, j]), cmul(a[i, 1], b[1, j])) for i, j in INDEX}


def mat_mul_h(a, b):
    return {(i, j): cadd(cmul_conj(a[i, 0], b[j, 0]), cmul_conj(a[i, 1], b[j, 1])) for i, j in INDEX}


def mat_h_mul(a, b):
    return {(i, j): cadd(cmul_conj(b[0, j], a[0, i]), cmul_conj(b[1, j], a[1, i])) for i, j in INDEX}


def sq(a):
    return a[0] * a[0] + a[1] * a[1]


def split_dot(left, right, dims):
    high = left.astype(jnp.bfloat16)
    low = (left - high.astype(jnp.float32)).astype(jnp.bfloat16)
    both = jnp.concatenate([high, low], axis=0)
    out = lax.dot_general(both, right, (dims, ((), ())), preferred_element_type=jnp.float32)
    return out[: left.shape[0]] + out[left.shape[0] :]


def fill_onehot(pairs_ref, onehot_ref):
    stations = onehot_ref.shape[0]
    baselines = pairs_ref.shape[1]
    for half in range(2):
        ids = pairs_ref[half : half + 1, :]
        for base in range(0, stations, LANES):
            station = lax.broadcasted_iota(jnp.int32, (LANES, baselines), 0) + base
            hit = jnp.where(station == ids, 1.0, 0.0).astype(jnp.bfloat16)
            onehot_ref[base : base + LANES, half * baselines : (half + 1) * baselines] = hit


def read_rows(ref, dirs, k, base, width):
    def one(part, i, j):
        row = comp(part, i, j) * dirs + k
        return jnp.broadcast_to(ref[row : row + 1, base : base + width], (SUBLANES, width))

    return {(i, j): (one(0, i, j), one(1, i, j)) for i, j in INDEX}


def native_to_rows(block, dirs, store):
    for k in range(dirs):
        for part in range(2):
            for i in range(2):
                value = block(k, part, i)
                for j in range(2):
                    store(comp(part, i, j) * dirs + k, value[j : j + 1, :])


def store_chunks(ref, row, value):
    width = ref.shape[2]
    for chunk in range(ref.shape[0]):
        ref[chunk, row : row + value.shape[0], :] = value[:, chunk * width : (chunk + 1) * width]


def prepare_kernel(basis_ref, dual_ref, coeffs_ref, known_ref, lag_ref):
    terms, dirs = coeffs_ref.shape[:2]

    def known(k, part, i):
        total = coeffs_ref[0, k, part, i] * basis_ref[0, 0]
        for m in range(1, terms):
            total = total + coeffs_ref[m, k, part, i] * basis_ref[0, m]
        return RHO * total - dual_ref[k, part, i]

    native_to_rows(known, dirs, lambda row, value: store_chunks(known_ref, row, value))
    native_to_rows(
        lambda k, part, i: dual_ref[k, part, i] * (1.0 / RHO), dirs,
        lambda row, value: store_chunks(lag_ref, row, value),
    )


def model_body(parity_ref, jones, onehot_ref, coher_ref, gathered_ref, mine_ref, other_ref):
    dirs = coher_ref.shape[0]
    times, baselines = coher_ref.shape[-2:]
    gathered_ref[...] = split_dot(jones, onehot_ref[...], ((1,), (0,)))
    first = parity_ref[...] == 0
    for base in range(0, baselines, LANES):
        lanes = slice(base, base + LANES)
        for time in range(0, times, SUBLANES):
            rows = slice(time, time + SUBLANES)
            total = None
            for k in range(dirs):
                jones_p = read_rows(gathered_ref, dirs, k, base, LANES)
                jones_q = read_rows(gathered_ref, dirs, k, baselines + base, LANES)
                coher = {(i, j): tuple(coher_ref[k, part, i, j, rows, lanes] for part in range(2)) for i, j in INDEX}
                model = mat_mul(jones_p, mat_mul_h(coher, jones_q))
                total = model if total is None else {ij: cadd(total[ij], model[ij]) for ij in INDEX}
            for i, j in INDEX:
                real, imag = total[i, j]
                mine_ref[i, j, rows, lanes] = jnp.where(first, real, imag)
                other_ref[i, j, rows, lanes] = jnp.where(first, imag, real)


def first_model_kernel(
    parity_ref, jones_hbm, pairs_hbm, coher_hbm, gathered_ref, mine_ref, other_ref,
    onehot_ref, rows_ref, jones_ref, pairs_ref, coher_ref, sems,
):
    copies = [
        pltpu.make_async_copy(source, target, sems.at[at])
        for at, (source, target) in enumerate(
            ((pairs_hbm, pairs_ref), (jones_hbm, jones_ref), (coher_hbm, coher_ref))
        )
    ]
    for copy in copies:
        copy.start()
    copies[0].wait()
    fill_onehot(pairs_ref, onehot_ref)
    copies[1].wait()

    def store(row, value):
        rows_ref[row : row + 1, :] = value

    native_to_rows(lambda k, part, i: jones_ref[k, part, i], coher_ref.shape[0], store)
    copies[2].wait()
    model_body(parity_ref, rows_ref[...], onehot_ref, coher_ref, gathered_ref, mine_ref, other_ref)


def model_kernel(parity_ref, jones_ref, pairs_ref, coher_ref, gathered_ref, mine_ref, other_ref, onehot_ref):
    fill_onehot(pairs_ref, onehot_ref)
    model_body(parity_ref, jones_ref[...], onehot_ref, coher_ref, gathered_ref, mine_ref, other_ref)


def reduced_terms(gathered_ref, coher_ref, left_ref, terms_of):
    dirs = coher_ref.shape[0]
    times, baselines = coher_ref.shape[-2:]
    for base in range(0, baselines, LANES):
        lanes = slice(base, base + LANES)
        for k in range(dirs):
            jones_p = read_rows(gathered_ref, dirs, k, base, LANES)
            jones_q = read_rows(gathered_ref, dirs, k, baselines + base, LANES)
            sums = None
            for index, time in enumerate(range(0, times, SUBLANES)):
                rows = slice(time, time + SUBLANES)
                coher = {(i, j): tuple(coher_ref[k, part, i, j, rows, lanes] for part in range(2)) for i, j in INDEX}
                terms = terms_of(mat_mul_h(coher, jones_q), mat_mul(jones_p, coher), base, index)
                sums = terms if sums is None else [a + b for a, b in zip(sums, terms)]
            count = len(sums) // 2
            for at, term in enumerate(sums):
                row = (at % count) * dirs + k
                offset = base + (at // count) * baselines
                left_ref[row : row + 1, offset : offset + LANES] = jnp.sum(term, axis=0, keepdims=True)


def normal_kernel(gathered_ref, pairs_ref, coher_ref, base_ref, onehot_ref, normal_ref, left_ref):
    dirs = coher_ref.shape[0]
    fill_onehot(pairs_ref, onehot_ref)

    def terms_of(along, ahead, base, index):
        cross_p = cadd(cmul_conj(along[0, 0], along[1, 0]), cmul_conj(along[0, 1], along[1, 1]))
        cross_q = cadd(cmul_conj(ahead[0, 1], ahead[0, 0]), cmul_conj(ahead[1, 1], ahead[1, 0]))
        return [
            sq(along[0, 0]) + sq(along[0, 1]),
            sq(along[1, 0]) + sq(along[1, 1]),
            cross_p[0],
            cross_p[1],
            sq(ahead[0, 0]) + sq(ahead[1, 0]),
            sq(ahead[0, 1]) + sq(ahead[1, 1]),
            cross_q[0],
            cross_q[1],
        ]

    reduced_terms(gathered_ref, coher_ref, normal_ref, terms_of)

    def group(ref, at):
        return ref[at * dirs : (at + 1) * dirs, :]

    jones = {(i, j): (group(gathered_ref, comp(0, i, j)), group(gathered_ref, comp(1, i, j))) for i, j in INDEX}
    diag0, diag1 = group(normal_ref, 0), group(normal_ref, 1)
    off = (group(normal_ref, 2), group(normal_ref, 3))
    off_c = (off[0], -off[1])
    for i in range(2):
        left, right = jones[i, 0], jones[i, 1]
        col0 = cadd((left[0] * diag0, left[1] * diag0), cmul(right, off_c))
        col1 = cadd(cmul(left, off), (right[0] * diag1, right[1] * diag1))
        for j, col in ((0, col0), (1, col1)):
            for part in range(2):
                at = comp(part, i, j) * dirs
                left_ref[at : at + dirs, :] = col[part]
    left_ref[8 * dirs :, :] = normal_ref[...]
    sums = split_dot(left_ref[...], onehot_ref[...], ((1,), (1,)))
    store_chunks(base_ref, 0, sums[: 8 * dirs])
    m00 = sums[8 * dirs : 9 * dirs] + RHO
    m11 = sums[9 * dirs : 10 * dirs] + RHO
    m01 = (sums[10 * dirs : 11 * dirs], sums[11 * dirs : 12 * dirs])
    scale = 1.0 / (m00 * m11 - sq(m01))
    store_chunks(base_ref, 8 * dirs, m11 * scale)
    store_chunks(base_ref, 9 * dirs, m00 * scale)
    store_chunks(base_ref, 10 * dirs, -m01[0] * scale)
    store_chunks(base_ref, 11 * dirs, -m01[1] * scale)


def right_kernel(
    parity_ref, gathered_ref, pairs_ref, coher_ref, vis_ref, mine_ref, other_ref, base_ref, sums_ref,
    onehot_ref, left_ref,
):
    dirs = coher_ref.shape[0]
    fill_onehot(pairs_ref, onehot_ref)
    first = parity_ref[...] == 0

    def residual(base, index):
        lanes = slice(base, base + LANES)
        rows = slice(index * SUBLANES, (index + 1) * SUBLANES)
        piece = {}
        for i, j in INDEX:
            mine = mine_ref[i, j, rows, lanes]
            other = other_ref[i, j, rows, lanes]
            piece[i, j] = (
                vis_ref[0, i, j, rows, lanes] - jnp.where(first, mine, other),
                vis_ref[1, i, j, rows, lanes] - jnp.where(first, other, mine),
            )
        return piece

    kept = {}

    def terms_of(along, ahead, base, index):
        if (base, index) not in kept:
            kept[base, index] = residual(base, index)
        piece = kept[base, index]
        right_p = mat_mul_h(piece, along)
        right_q = mat_h_mul(piece, ahead)
        return [side[ij][part] for side in (right_p, right_q) for part in range(2) for ij in INDEX]

    reduced_terms(gathered_ref, coher_ref, left_ref, terms_of)
    sums = split_dot(left_ref[...], onehot_ref[...], ((1,), (1,)))
    rows, width = 8 * dirs, sums_ref.shape[2]
    for chunk in range(sums_ref.shape[0]):
        part = sums[:, chunk * width : (chunk + 1) * width]
        sums_ref[chunk, :rows, :] = base_ref[chunk, :rows, :] + part
        sums_ref[chunk, rows:, :] = base_ref[chunk, rows:, :]


def solve(sums, known, dirs):
    i00, i11, re01, im01 = (sums(at * dirs) for at in range(8, 12))
    i01, i10 = (re01, im01), (re01, -im01)
    out = {}
    for i in range(2):
        n = []
        for j in range(2):
            at = [comp(part, i, j) * dirs for part in range(2)]
            n.append(tuple(sums(a) + known(a) for a in at))
        left = cadd((n[0][0] * i00, n[0][1] * i00), cmul(n[1], i10))
        right = cadd(cmul(n[0], i01), (n[1][0] * i11, n[1][1] * i11))
        for part in range(2):
            out[comp(part, i, 0) * dirs] = left[part]
            out[comp(part, i, 1) * dirs] = right[part]
    return out


def first_update_kernel(basis_ref, sums_ref, known_ref, lag_ref, jones_ref, unit_ref):
    dirs = sums_ref.shape[1] // 12
    chunks, rows, width = known_ref.shape
    terms = basis_ref.shape[1]
    for chunk in range(chunks):
        out = solve(
            lambda a: sums_ref[chunk, a : a + dirs, :], lambda a: known_ref[chunk, a : a + dirs, :], dirs
        )
        for a, value in out.items():
            jones_ref[a : a + dirs, chunk * width : (chunk + 1) * width] = value
            at = chunk * rows + a
            unit_ref[at : at + dirs, :] = value + lag_ref[chunk, a : a + dirs, :]
    unit_ref[chunks * rows :, :] = jnp.zeros((SUBLANES, width), jnp.float32)
    unit_ref[chunks * rows : chunks * rows + 1, :terms] = basis_ref[...]


def solve_next(sums, consensus, before, dirs):
    out = solve(sums, lambda a: RHO * (2.0 * consensus(a) - before(a)), dirs)
    return out, {a: value + (before(a) - consensus(a)) for a, value in out.items()}


def solve_chunk(chunk, sums_ref, consensus_ref, before_ref):
    dirs = sums_ref.shape[1] // 12

    def rows(ref):
        return lambda a: ref[chunk, a : a + dirs, :]

    return solve_next(rows(sums_ref), rows(consensus_ref), rows(before_ref), dirs)


def update_kernel(sums_ref, consensus_ref, before_ref, jones_ref, shared_ref):
    dirs, width = sums_ref.shape[1] // 12, sums_ref.shape[2]
    for chunk in range(sums_ref.shape[0]):
        jones, shared = solve_chunk(chunk, sums_ref, consensus_ref, before_ref)
        for a in jones:
            jones_ref[a : a + dirs, chunk * width : (chunk + 1) * width] = jones[a]
            shared_ref[chunk, a : a + dirs, :] = shared[a]


def store_native(chunk, width, dirs, rows, ref):
    for part in range(2):
        for i, j in INDEX:
            value = rows[comp(part, i, j) * dirs]
            for k in range(dirs):
                ref[k, part, i, j : j + 1, chunk * width : (chunk + 1) * width] = value[k : k + 1, :]


def last_update_kernel(sums_ref, consensus_ref, before_ref, jones_ref, shared_ref):
    dirs, width = sums_ref.shape[1] // 12, sums_ref.shape[2]
    for chunk in range(sums_ref.shape[0]):
        jones, shared = solve_chunk(chunk, sums_ref, consensus_ref, before_ref)
        store_native(chunk, width, dirs, jones, jones_ref)
        store_native(chunk, width, dirs, shared, shared_ref)


def weighted(matrix, g, values):
    total = None
    for f, value in enumerate(values):
        weight = jnp.broadcast_to(matrix[g : g + 1, f : f + 1], value.shape[-2:])
        total = weight * value if total is None else total + weight * value
    return total


def gathered_update_kernel(sums_ref, *refs):
    units, (jones_ref, shared_ref, spread_ref, weights_ref) = refs[:-4], refs[-4:]
    dirs = sums_ref.shape[1] // 12
    chunks, _, width = sums_ref.shape
    rows = 8 * dirs
    terms = weights_ref.shape[0]
    bands = len(units)
    hi = lax.Precision.HIGHEST
    at = chunks * rows
    basis = jnp.concatenate([ref[at : at + 1, :terms] for ref in units], axis=0)
    gram = lax.dot_general(basis, basis, (((0,), (0,)), ((), ())), precision=hi, preferred_element_type=jnp.float32)
    row = lax.broadcasted_iota(jnp.int32, (terms, terms), 0)
    col = lax.broadcasted_iota(jnp.int32, (terms, terms), 1)
    gram = gram + jnp.where(row == col, RIDGE * bands, 0.0)
    inverse = jnp.where(row == col, 1.0, 0.0)
    for t in range(terms):
        scale = 1.0 / gram[t : t + 1, t : t + 1]
        g_row = gram[t : t + 1, :] * scale
        i_row = inverse[t : t + 1, :] * scale
        factor = gram[:, t : t + 1]
        here = row == t
        gram = jnp.where(here, g_row, gram - factor * g_row)
        inverse = jnp.where(here, i_row, inverse - factor * i_row)
    weights = lax.dot_general(inverse, basis, (((1,), (1,)), ((), ())), precision=hi, preferred_element_type=jnp.float32)
    spread = jnp.dot(basis, weights, precision=hi, preferred_element_type=jnp.float32)
    spread_ref[...] = spread
    weights_ref[...] = weights
    for chunk in range(chunks):
        jones, shared = solve_gathered(chunk, spread, sums_ref, units, rows)
        for a in jones:
            jones_ref[a : a + dirs, chunk * width : (chunk + 1) * width] = jones[a]
            shared_ref[chunk * rows + a : chunk * rows + a + dirs, :] = shared[a]


def solve_gathered(chunk, spread, sums_ref, units, rows):
    dirs = sums_ref.shape[1] // 12
    base = chunk * rows
    values = [ref[base : base + rows, :] for ref in units]
    consensus = weighted(spread, 0, values)
    return solve_next(
        lambda a: sums_ref[chunk, a : a + dirs, :],
        lambda a: consensus[a : a + dirs],
        lambda a: values[0][a : a + dirs],
        dirs,
    )


def partial_consensus_kernel(spread_ref, *refs):
    units, out_ref = refs[:-1], refs[-1]
    rows = out_ref.shape[0]
    spread = spread_ref[...]
    step = 4 * SUBLANES
    for base in range(0, rows, step):
        out_ref[base : base + step, :] = weighted(spread, 0, [ref[base : base + step, :] for ref in units])


def gathered_last_kernel(spread_ref, sums_ref, own_ref, partial_ref, *refs):
    units, (jones_ref, shared_ref) = refs[:-2], refs[-2:]
    dirs, width = sums_ref.shape[1] // 12, sums_ref.shape[2]
    rows = 8 * dirs
    spread = spread_ref[0:1, spread_ref.shape[0] - len(units) :]
    for chunk in range(sums_ref.shape[0]):
        base = chunk * rows
        rest = weighted(spread, 0, [ref[base : base + rows, :] for ref in units])
        consensus = partial_ref[base : base + rows, :] + rest
        jones, shared = solve_next(
            lambda a: sums_ref[chunk, a : a + dirs, :],
            lambda a: consensus[a : a + dirs],
            lambda a: own_ref[base + a : base + a + dirs, :],
            dirs,
        )
        for a in jones:
            jones_ref[a : a + dirs, chunk * width : (chunk + 1) * width] = jones[a]
        store_native(chunk, width, dirs, shared, shared_ref)


def native_kernel(rows_ref, out_ref):
    dirs = out_ref.shape[0]
    rows = {a: rows_ref[a : a + dirs, :] for a in range(0, 8 * dirs, dirs)}
    store_native(0, rows_ref.shape[1], dirs, rows, out_ref)


def partial_coeffs_kernel(weights_ref, *refs):
    units, out_ref = refs[:-1], refs[-1]
    weights = weights_ref[...]
    for k in range(out_ref.shape[1]):
        for part in range(2):
            for i in range(2):
                values = [ref[k, part, i] for ref in units]
                for m in range(weights.shape[0]):
                    out_ref[m, k, part, i] = weighted(weights, m, values)


def final_kernel(basis_ref, weights_ref, own_ref, partial_ref, *refs):
    units, (coeffs_hbm, dual_hbm, coeffs_ref, dual_ref, sems) = refs[:-5], refs[-5:]
    terms, dirs = coeffs_ref.shape[:2]
    weights = weights_ref[:, weights_ref.shape[1] - len(units) :]
    copies = []
    for k in range(dirs):
        for part in range(2):
            for i in range(2):
                values = [ref[k, part, i] for ref in units]
                consensus = None
                for m in range(terms):
                    total = partial_ref[m, k, part, i] + weighted(weights, m, values)
                    coeffs_ref[m, k, part, i] = total
                    share = total * jnp.broadcast_to(basis_ref[0:1, m : m + 1], total.shape)
                    consensus = share if consensus is None else consensus + share
                dual_ref[k, part, i] = RHO * (own_ref[k, part, i] - consensus)
        copies.append(pltpu.make_async_copy(coeffs_ref.at[:, k], coeffs_hbm.at[:, k], sems.at[k]))
        copies[-1].start()
    copies.append(pltpu.make_async_copy(dual_ref, dual_hbm, sems.at[dirs]))
    copies[-1].start()
    for copy in copies:
        copy.wait()


def struct(*shape, dtype=jnp.float32):
    return jax.ShapeDtypeStruct(shape, dtype)


def call(kernel, out_shape, first, args, scratch=(), space=VMEM, out_space=VMEM):
    many = isinstance(out_shape, (tuple, list))
    return pl.pallas_call(
        kernel,
        out_shape=out_shape,
        in_specs=[space if at else first for at in range(len(args))],
        out_specs=tuple(out_space for _ in out_shape) if many else out_space,
        scratch_shapes=list(scratch),
        compiler_params=PARAMS,
    )(*args)


def swap(value, axis, bit):
    size = lax.axis_size(axis)
    return lax.ppermute(value, axis, [(i, i ^ bit) for i in range(size)])


def sum_over_dir(mine, other):
    size = lax.axis_size("dir")
    mine = mine + swap(other, "dir", 1)
    bit = 2
    while bit < size:
        far = swap(mine, "dir", bit)
        mine = mine + far
        bit *= 2
    return mine, swap(mine, "dir", 1)


def gather_bands(value):
    half = lax.axis_size("band") // 2
    far = swap(value, "band", half)
    near = [value]
    for bit in range(1, half):
        near.append(swap(value, "band", bit))
    passed = [far]
    for bit in range(1, half):
        passed.append(swap(far, "band", bit))
    return near + passed


def reduce_bands(shared, row, factor):
    sums = lax.psum(row.reshape((-1,) + (1,) * shared.ndim) * shared[None], "band")
    flat = sums.reshape(sums.shape[0], -1)
    return jax.scipy.linalg.cho_solve((factor, True), flat).reshape(sums.shape)


def local(visibilities, coherencies, jones_start, dual_start, consensus_start, freq_basis, pairs):
    row = freq_basis[0]
    terms = row.shape[0]
    bands = lax.axis_size("band")
    vis, coher = visibilities[0], coherencies[0]
    native = jones_start.shape[1:]
    dirs, stations = native[0], native[-1]
    times, baselines = coher.shape[-2:]
    rows = 8 * dirs
    parity = jnp.broadcast_to((lax.axis_index("dir") % 2).astype(jnp.int32), (SUBLANES, LANES))
    chunked = stations % (bands * LANES) == 0 and bands > 2 and bands & (bands - 1) == 0
    hi = lax.Precision.HIGHEST
    width = stations // bands if chunked else LANES
    chunks = stations // width
    half = struct(2, 2, times, baselines)
    flat = struct(rows, stations)
    spread_rows = struct(chunks, rows, width)
    onehot = pltpu.VMEM((stations, 2 * baselines), jnp.bfloat16)
    left = pltpu.VMEM((12 * dirs, 2 * baselines), jnp.float32)
    model_out = (struct(rows, 2 * baselines), half, half)

    if not chunked:
        gram = lax.psum(row[:, None] * row[None, :], "band") + RIDGE * bands * jnp.eye(terms, dtype=jnp.float32)
        factor = jnp.linalg.cholesky(gram)

    def model(jones):
        return call(model_kernel, model_out, VMEM, (parity, jones, pairs, coher), [onehot])

    def station_sums(gathered, mine, other):
        base = call(
            normal_kernel, struct(chunks, 12 * dirs, width), VMEM, (gathered, pairs, coher),
            [onehot, pltpu.VMEM((4 * dirs, 2 * baselines), jnp.float32), left],
        )
        mine, other = sum_over_dir(mine, other)
        return call(
            right_kernel, struct(chunks, 12 * dirs, width), VMEM,
            (parity, gathered, pairs, coher, vis, mine, other, base),
            [onehot, pltpu.VMEM((rows, 2 * baselines), jnp.float32)],
        )

    def share(shared):
        coeffs = reduce_bands(shared, row, factor)
        return coeffs, jnp.tensordot(row, coeffs, axes=(0, 0), precision=hi)

    started = call(
        first_model_kernel, model_out, VMEM,
        (parity, *(pltpu.with_memory_space_constraint(x, pltpu.HBM) for x in (jones_start[0], pairs, coher))),
        [
            onehot,
            pltpu.VMEM((rows, stations), jnp.float32),
            pltpu.VMEM(native, jnp.float32),
            pltpu.VMEM(pairs.shape, pairs.dtype),
            pltpu.VMEM(coher.shape, jnp.float32),
            pltpu.SemaphoreType.DMA((3,)),
        ],
        HBM,
    )
    known, lag = call(prepare_kernel, (spread_rows,) * 2, SMEM, (freq_basis, dual_start[0], consensus_start))
    jones, unit = call(
        first_update_kernel, (flat, struct(stations * rows // width + SUBLANES, width)), VMEM,
        (freq_basis, station_sums(*started), known, lag),
    )
    if chunked:
        early = bands // 2 + 1
        units = gather_bands(unit)
        started = model(jones)
        sums = station_sums(*started)
        jones, unit, spread, weights = call(
            gathered_update_kernel,
            (flat, struct(chunks * rows, width), struct(bands, bands), struct(terms, bands)), VMEM, (sums, *units),
        )
        units = gather_bands(unit)
        started = model(jones)
        sums = station_sums(*started)
        partial = call(partial_consensus_kernel, struct(chunks * rows, width), VMEM, (spread, *units[:early]))
        jones, shared = call(
            gathered_last_kernel, (flat, struct(*native)), VMEM, (spread, sums, unit, partial, *units[early:])
        )
        jones = call(native_kernel, struct(*native), VMEM, (jones,))
        units = gather_bands(shared)
        partial = call(partial_coeffs_kernel, struct(terms, *native), VMEM, (weights, *units[:early]))
        coeffs, dual = call(
            final_kernel, (struct(terms, *native), struct(*native)), VMEM,
            (freq_basis, weights, shared, partial, *units[early:]),
            [
                pltpu.VMEM((terms, *native), jnp.float32),
                pltpu.VMEM(native, jnp.float32),
                pltpu.SemaphoreType.DMA((dirs + 1,)),
            ],
            out_space=HBM,
        )
    else:
        shared = unit[: chunks * rows].reshape(spread_rows.shape)
        for _ in range(ITERS - 2):
            consensus = share(shared)[1]
            sums = station_sums(*model(jones))
            jones, shared = call(update_kernel, (flat, spread_rows), VMEM, (sums, consensus, shared))
        consensus = share(shared)[1]
        sums = station_sums(*model(jones))
        jones, shared = call(last_update_kernel, (struct(*native),) * 2, VMEM, (sums, consensus, shared))
        coeffs, consensus = share(shared)
        dual = RHO * (shared - consensus)
    return jones[None], dual[None], coeffs


def solution(mesh):
    in_specs = (
        P("band", None, None, None, None, None),
        P("band", "dir", None, None, None, None, None),
        P("band", "dir", None, None, None, None),
        P("band", "dir", None, None, None, None),
        P(None, "dir", None, None, None, None),
        P("band", None),
        P(),
    )
    out_specs = (
        P("band", "dir", None, None, None, None),
        P("band", "dir", None, None, None, None),
        P(None, "dir", None, None, None, None),
    )

    return jax.shard_map(local, mesh=mesh, in_specs=in_specs, out_specs=out_specs, check_vma=False)
```

```python
import jax
import jax.numpy as jnp
from jax import lax
from jax.experimental import pallas as pl
from jax.experimental.pallas import tpu as pltpu
from jax.sharding import PartitionSpec as P

ITERS = 3
RHO = 5.0
RIDGE = 0.25
LANES = 128
SUBLANES = 8

VMEM = pl.BlockSpec(memory_space=pltpu.VMEM)
SMEM = pl.BlockSpec(memory_space=pltpu.SMEM)
HBM = pl.BlockSpec(memory_space=pltpu.HBM)
PARAMS = pltpu.CompilerParams(vmem_limit_bytes=16 * 1024 * 1024)

INDEX = ((0, 0), (0, 1), (1, 0), (1, 1))


def comp(part, i, j):
    return part * 4 + i * 2 + j


def cadd(a, b):
    return (a[0] + b[0], a[1] + b[1])


def cmul(a, b):
    return (a[0] * b[0] - a[1] * b[1], a[0] * b[1] + a[1] * b[0])


def cmul_conj(a, b):
    return (a[0] * b[0] + a[1] * b[1], a[1] * b[0] - a[0] * b[1])


def mat_mul(a, b):
    return {(i, j): cadd(cmul(a[i, 0], b[0, j]), cmul(a[i, 1], b[1, j])) for i, j in INDEX}


def mat_mul_h(a, b):
    return {(i, j): cadd(cmul_conj(a[i, 0], b[j, 0]), cmul_conj(a[i, 1], b[j, 1])) for i, j in INDEX}


def mat_h_mul(a, b):
    return {(i, j): cadd(cmul_conj(b[0, j], a[0, i]), cmul_conj(b[1, j], a[1, i])) for i, j in INDEX}


def sq(a):
    return a[0] * a[0] + a[1] * a[1]


def split_dot(left, right, dims):
    high = left.astype(jnp.bfloat16)
    low = (left - high.astype(jnp.float32)).astype(jnp.bfloat16)
    both = jnp.concatenate([high, low], axis=0)
    out = lax.dot_general(both, right, (dims, ((), ())), preferred_element_type=jnp.float32)
    return out[: left.shape[0]] + out[left.shape[0] :]


def fill_onehot(pairs_ref, onehot_ref):
    stations = onehot_ref.shape[0]
    baselines = pairs_ref.shape[1]
    for half in range(2):
        ids = pairs_ref[half : half + 1, :]
        for base in range(0, stations, LANES):
            station = lax.broadcasted_iota(jnp.int32, (LANES, baselines), 0) + base
            hit = jnp.where(station == ids, 1.0, 0.0).astype(jnp.bfloat16)
            onehot_ref[base : base + LANES, half * baselines : (half + 1) * baselines] = hit


def read_rows(ref, dirs, k, base, width):
    def one(part, i, j):
        row = comp(part, i, j) * dirs + k
        return jnp.broadcast_to(ref[row : row + 1, base : base + width], (SUBLANES, width))

    return {(i, j): (one(0, i, j), one(1, i, j)) for i, j in INDEX}


def native_to_rows(block, dirs, store):
    for k in range(dirs):
        for part in range(2):
            for i in range(2):
                value = block(k, part, i)
                for j in range(2):
                    store(comp(part, i, j) * dirs + k, value[j : j + 1, :])


def store_chunks(ref, row, value):
    width = ref.shape[2]
    for chunk in range(ref.shape[0]):
        ref[chunk, row : row + value.shape[0], :] = value[:, chunk * width : (chunk + 1) * width]


def prepare_kernel(basis_ref, dual_ref, coeffs_ref, known_ref, lag_ref):
    terms, dirs = coeffs_ref.shape[:2]

    def known(k, part, i):
        total = coeffs_ref[0, k, part, i] * basis_ref[0, 0]
        for m in range(1, terms):
            total = total + coeffs_ref[m, k, part, i] * basis_ref[0, m]
        return RHO * total - dual_ref[k, part, i]

    native_to_rows(known, dirs, lambda row, value: store_chunks(known_ref, row, value))
    native_to_rows(
        lambda k, part, i: dual_ref[k, part, i] * (1.0 / RHO), dirs,
        lambda row, value: store_chunks(lag_ref, row, value),
    )


def model_body(parity_ref, jones, onehot_ref, coher_ref, gathered_ref, mine_ref, other_ref):
    dirs = coher_ref.shape[0]
    times, baselines = coher_ref.shape[-2:]
    gathered_ref[...] = split_dot(jones, onehot_ref[...], ((1,), (0,)))
    first = parity_ref[...] == 0
    for base in range(0, baselines, LANES):
        lanes = slice(base, base + LANES)
        for time in range(0, times, SUBLANES):
            rows = slice(time, time + SUBLANES)
            total = None
            for k in range(dirs):
                jones_p = read_rows(gathered_ref, dirs, k, base, LANES)
                jones_q = read_rows(gathered_ref, dirs, k, baselines + base, LANES)
                coher = {(i, j): tuple(coher_ref[k, part, i, j, rows, lanes] for part in range(2)) for i, j in INDEX}
                model = mat_mul(jones_p, mat_mul_h(coher, jones_q))
                total = model if total is None else {ij: cadd(total[ij], model[ij]) for ij in INDEX}
            for i, j in INDEX:
                real, imag = total[i, j]
                mine_ref[i, j, rows, lanes] = jnp.where(first, real, imag)
                other_ref[i, j, rows, lanes] = jnp.where(first, imag, real)


def first_model_kernel(
    parity_ref, jones_hbm, pairs_hbm, coher_hbm, gathered_ref, mine_ref, other_ref,
    onehot_ref, rows_ref, jones_ref, pairs_ref, coher_ref, sems,
):
    copies = [
        pltpu.make_async_copy(source, target, sems.at[at])
        for at, (source, target) in enumerate(
            ((pairs_hbm, pairs_ref), (jones_hbm, jones_ref), (coher_hbm, coher_ref))
        )
    ]
    for copy in copies:
        copy.start()
    copies[0].wait()
    fill_onehot(pairs_ref, onehot_ref)
    copies[1].wait()

    def store(row, value):
        rows_ref[row : row + 1, :] = value

    native_to_rows(lambda k, part, i: jones_ref[k, part, i], coher_ref.shape[0], store)
    copies[2].wait()
    model_body(parity_ref, rows_ref[...], onehot_ref, coher_ref, gathered_ref, mine_ref, other_ref)


def model_kernel(parity_ref, jones_ref, pairs_ref, coher_ref, gathered_ref, mine_ref, other_ref, onehot_ref):
    fill_onehot(pairs_ref, onehot_ref)
    model_body(parity_ref, jones_ref[...], onehot_ref, coher_ref, gathered_ref, mine_ref, other_ref)


def reduced_terms(gathered_ref, coher_ref, left_ref, terms_of):
    dirs = coher_ref.shape[0]
    times, baselines = coher_ref.shape[-2:]
    for base in range(0, baselines, LANES):
        lanes = slice(base, base + LANES)
        for k in range(dirs):
            jones_p = read_rows(gathered_ref, dirs, k, base, LANES)
            jones_q = read_rows(gathered_ref, dirs, k, baselines + base, LANES)
            sums = None
            for index, time in enumerate(range(0, times, SUBLANES)):
                rows = slice(time, time + SUBLANES)
                coher = {(i, j): tuple(coher_ref[k, part, i, j, rows, lanes] for part in range(2)) for i, j in INDEX}
                terms = terms_of(mat_mul_h(coher, jones_q), mat_mul(jones_p, coher), base, index)
                sums = terms if sums is None else [a + b for a, b in zip(sums, terms)]
            count = len(sums) // 2
            for at, term in enumerate(sums):
                row = (at % count) * dirs + k
                offset = base + (at // count) * baselines
                left_ref[row : row + 1, offset : offset + LANES] = jnp.sum(term, axis=0, keepdims=True)


def normal_kernel(gathered_ref, pairs_ref, coher_ref, base_ref, onehot_ref, normal_ref, left_ref):
    dirs = coher_ref.shape[0]
    fill_onehot(pairs_ref, onehot_ref)

    def terms_of(along, ahead, base, index):
        cross_p = cadd(cmul_conj(along[0, 0], along[1, 0]), cmul_conj(along[0, 1], along[1, 1]))
        cross_q = cadd(cmul_conj(ahead[0, 1], ahead[0, 0]), cmul_conj(ahead[1, 1], ahead[1, 0]))
        return [
            sq(along[0, 0]) + sq(along[0, 1]),
            sq(along[1, 0]) + sq(along[1, 1]),
            cross_p[0],
            cross_p[1],
            sq(ahead[0, 0]) + sq(ahead[1, 0]),
            sq(ahead[0, 1]) + sq(ahead[1, 1]),
            cross_q[0],
            cross_q[1],
        ]

    reduced_terms(gathered_ref, coher_ref, normal_ref, terms_of)

    def group(ref, at):
        return ref[at * dirs : (at + 1) * dirs, :]

    jones = {(i, j): (group(gathered_ref, comp(0, i, j)), group(gathered_ref, comp(1, i, j))) for i, j in INDEX}
    diag0, diag1 = group(normal_ref, 0), group(normal_ref, 1)
    off = (group(normal_ref, 2), group(normal_ref, 3))
    off_c = (off[0], -off[1])
    for i in range(2):
        left, right = jones[i, 0], jones[i, 1]
        col0 = cadd((left[0] * diag0, left[1] * diag0), cmul(right, off_c))
        col1 = cadd(cmul(left, off), (right[0] * diag1, right[1] * diag1))
        for j, col in ((0, col0), (1, col1)):
            for part in range(2):
                at = comp(part, i, j) * dirs
                left_ref[at : at + dirs, :] = col[part]
    left_ref[8 * dirs :, :] = normal_ref[...]
    sums = split_dot(left_ref[...], onehot_ref[...], ((1,), (1,)))
    store_chunks(base_ref, 0, sums[: 8 * dirs])
    m00 = sums[8 * dirs : 9 * dirs] + RHO
    m11 = sums[9 * dirs : 10 * dirs] + RHO
    m01 = (sums[10 * dirs : 11 * dirs], sums[11 * dirs : 12 * dirs])
    scale = 1.0 / (m00 * m11 - sq(m01))
    store_chunks(base_ref, 8 * dirs, m11 * scale)
    store_chunks(base_ref, 9 * dirs, m00 * scale)
    store_chunks(base_ref, 10 * dirs, -m01[0] * scale)
    store_chunks(base_ref, 11 * dirs, -m01[1] * scale)


def right_kernel(
    parity_ref, gathered_ref, pairs_ref, coher_ref, vis_ref, mine_ref, other_ref, base_ref, sums_ref,
    onehot_ref, left_ref,
):
    dirs = coher_ref.shape[0]
    fill_onehot(pairs_ref, onehot_ref)
    first = parity_ref[...] == 0

    def residual(base, index):
        lanes = slice(base, base + LANES)
        rows = slice(index * SUBLANES, (index + 1) * SUBLANES)
        piece = {}
        for i, j in INDEX:
            mine = mine_ref[i, j, rows, lanes]
            other = other_ref[i, j, rows, lanes]
            piece[i, j] = (
                vis_ref[0, i, j, rows, lanes] - jnp.where(first, mine, other),
                vis_ref[1, i, j, rows, lanes] - jnp.where(first, other, mine),
            )
        return piece

    kept = {}

    def terms_of(along, ahead, base, index):
        if (base, index) not in kept:
            kept[base, index] = residual(base, index)
        piece = kept[base, index]
        right_p = mat_mul_h(piece, along)
        right_q = mat_h_mul(piece, ahead)
        return [side[ij][part] for side in (right_p, right_q) for part in range(2) for ij in INDEX]

    reduced_terms(gathered_ref, coher_ref, left_ref, terms_of)
    sums = split_dot(left_ref[...], onehot_ref[...], ((1,), (1,)))
    rows, width = 8 * dirs, sums_ref.shape[2]
    for chunk in range(sums_ref.shape[0]):
        part = sums[:, chunk * width : (chunk + 1) * width]
        sums_ref[chunk, :rows, :] = base_ref[chunk, :rows, :] + part
        sums_ref[chunk, rows:, :] = base_ref[chunk, rows:, :]


def solve(sums, known, dirs):
    i00, i11, re01, im01 = (sums(at * dirs) for at in range(8, 12))
    i01, i10 = (re01, im01), (re01, -im01)
    out = {}
    for i in range(2):
        n = []
        for j in range(2):
            at = [comp(part, i, j) * dirs for part in range(2)]
            n.append(tuple(sums(a) + known(a) for a in at))
        left = cadd((n[0][0] * i00, n[0][1] * i00), cmul(n[1], i10))
        right = cadd(cmul(n[0], i01), (n[1][0] * i11, n[1][1] * i11))
        for part in range(2):
            out[comp(part, i, 0) * dirs] = left[part]
            out[comp(part, i, 1) * dirs] = right[part]
    return out


def first_update_kernel(basis_ref, sums_ref, known_ref, lag_ref, jones_ref, unit_ref):
    dirs = sums_ref.shape[1] // 12
    chunks, rows, width = known_ref.shape
    terms = basis_ref.shape[1]
    for chunk in range(chunks):
        out = solve(
            lambda a: sums_ref[chunk, a : a + dirs, :], lambda a: known_ref[chunk, a : a + dirs, :], dirs
        )
        for a, value in out.items():
            jones_ref[a : a + dirs, chunk * width : (chunk + 1) * width] = value
            at = chunk * rows + a
            unit_ref[at : at + dirs, :] = value + lag_ref[chunk, a : a + dirs, :]
    unit_ref[chunks * rows :, :] = jnp.zeros((SUBLANES, width), jnp.float32)
    unit_ref[chunks * rows : chunks * rows + 1, :terms] = basis_ref[...]


def solve_next(sums, consensus, before, dirs):
    out = solve(sums, lambda a: RHO * (2.0 * consensus(a) - before(a)), dirs)
    return out, {a: value + (before(a) - consensus(a)) for a, value in out.items()}


def solve_chunk(chunk, sums_ref, consensus_ref, before_ref):
    dirs = sums_ref.shape[1] // 12

    def rows(ref):
        return lambda a: ref[chunk, a : a + dirs, :]

    return solve_next(rows(sums_ref), rows(consensus_ref), rows(before_ref), dirs)


def update_kernel(sums_ref, consensus_ref, before_ref, jones_ref, shared_ref):
    dirs, width = sums_ref.shape[1] // 12, sums_ref.shape[2]
    for chunk in range(sums_ref.shape[0]):
        jones, shared = solve_chunk(chunk, sums_ref, consensus_ref, before_ref)
        for a in jones:
            jones_ref[a : a + dirs, chunk * width : (chunk + 1) * width] = jones[a]
            shared_ref[chunk, a : a + dirs, :] = shared[a]


def store_native(chunk, width, dirs, rows, ref):
    for part in range(2):
        for i, j in INDEX:
            value = rows[comp(part, i, j) * dirs]
            for k in range(dirs):
                ref[k, part, i, j : j + 1, chunk * width : (chunk + 1) * width] = value[k : k + 1, :]


def last_update_kernel(sums_ref, consensus_ref, before_ref, jones_ref, shared_ref):
    dirs, width = sums_ref.shape[1] // 12, sums_ref.shape[2]
    for chunk in range(sums_ref.shape[0]):
        jones, shared = solve_chunk(chunk, sums_ref, consensus_ref, before_ref)
        store_native(chunk, width, dirs, jones, jones_ref)
        store_native(chunk, width, dirs, shared, shared_ref)


def weighted(matrix, g, values):
    total = None
    for f, value in enumerate(values):
        weight = jnp.broadcast_to(matrix[g : g + 1, f : f + 1], value.shape[-2:])
        total = weight * value if total is None else total + weight * value
    return total


def basis_of(units, at, terms):
    return jnp.concatenate([ref[at : at + 1, :terms] for ref in units], axis=0)


def weights_kernel(basis_ref, weights_ref):
    terms, bands = weights_ref.shape
    hi = lax.Precision.HIGHEST
    basis = basis_ref[...]
    gram = lax.dot_general(basis, basis, (((0,), (0,)), ((), ())), precision=hi, preferred_element_type=jnp.float32)
    row = lax.broadcasted_iota(jnp.int32, (terms, terms), 0)
    col = lax.broadcasted_iota(jnp.int32, (terms, terms), 1)
    gram = gram + jnp.where(row == col, RIDGE * bands, 0.0)
    inverse = jnp.where(row == col, 1.0, 0.0)
    for t in range(terms):
        scale = 1.0 / gram[t : t + 1, t : t + 1]
        g_row = gram[t : t + 1, :] * scale
        i_row = inverse[t : t + 1, :] * scale
        factor = gram[:, t : t + 1]
        here = row == t
        gram = jnp.where(here, g_row, gram - factor * g_row)
        inverse = jnp.where(here, i_row, inverse - factor * i_row)
    weights_ref[...] = lax.dot_general(
        inverse, basis, (((1,), (1,)), ((), ())), precision=hi, preferred_element_type=jnp.float32
    )


def own_spread(basis):
    bands, terms = basis.shape
    entry = [
        [jnp.broadcast_to(basis[f : f + 1, m : m + 1], (SUBLANES, LANES)) for m in range(terms)] for f in range(bands)
    ]
    gram = {}
    for m in range(terms):
        for n in range(m, terms):
            total = None
            for f in range(bands):
                product = entry[f][m] * entry[f][n]
                total = product if total is None else total + product
            gram[m, n] = total + RIDGE * bands if m == n else total
    right = list(entry[0])
    scale = []
    for t in range(terms):
        scale.append(1.0 / gram[t, t])
        for m in range(t + 1, terms):
            factor = gram[t, m] * scale[t]
            right[m] = right[m] - factor * right[t]
            for n in range(m, terms):
                gram[m, n] = gram[m, n] - factor * gram[t, n]
    solved = [None] * terms
    for t in reversed(range(terms)):
        value = right[t]
        for n in range(t + 1, terms):
            value = value - gram[t, n] * solved[n]
        solved[t] = value * scale[t]
    out = []
    for f in range(bands):
        total = None
        for m in range(terms):
            product = solved[m] * entry[f][m]
            total = product if total is None else total + product
        out.append(total[0:1, 0:1])
    return jnp.concatenate(out, axis=1)


def gathered_update_kernel(sums_ref, *refs):
    units, (jones_ref, shared_ref, spread_ref, basis_ref) = refs[:-4], refs[-4:]
    dirs = sums_ref.shape[1] // 12
    chunks, _, width = sums_ref.shape
    rows = 8 * dirs
    basis = basis_of(units, chunks * rows, basis_ref.shape[1])
    basis_ref[...] = basis
    spread = own_spread(basis)
    spread_ref[...] = spread
    for chunk in range(chunks):
        jones, shared = solve_gathered(chunk, spread, sums_ref, units, rows)
        for a in jones:
            jones_ref[a : a + dirs, chunk * width : (chunk + 1) * width] = jones[a]
            shared_ref[chunk * rows + a : chunk * rows + a + dirs, :] = shared[a]


def solve_gathered(chunk, spread, sums_ref, units, rows):
    dirs = sums_ref.shape[1] // 12
    base = chunk * rows
    values = [ref[base : base + rows, :] for ref in units]
    consensus = weighted(spread, 0, values)
    return solve_next(
        lambda a: sums_ref[chunk, a : a + dirs, :],
        lambda a: consensus[a : a + dirs],
        lambda a: values[0][a : a + dirs],
        dirs,
    )


def partial_consensus_kernel(spread_ref, *refs):
    units, out_ref = refs[:-1], refs[-1]
    rows = out_ref.shape[0]
    spread = spread_ref[...]
    step = 4 * SUBLANES
    for base in range(0, rows, step):
        out_ref[base : base + step, :] = weighted(spread, 0, [ref[base : base + step, :] for ref in units])


def gathered_last_kernel(spread_ref, sums_ref, own_ref, partial_ref, *refs):
    units, (jones_ref, shared_ref) = refs[:-2], refs[-2:]
    dirs, width = sums_ref.shape[1] // 12, sums_ref.shape[2]
    rows = 8 * dirs
    spread = spread_ref[:, spread_ref.shape[1] - len(units) :]
    for chunk in range(sums_ref.shape[0]):
        base = chunk * rows
        rest = weighted(spread, 0, [ref[base : base + rows, :] for ref in units])
        consensus = partial_ref[base : base + rows, :] + rest
        jones, shared = solve_next(
            lambda a: sums_ref[chunk, a : a + dirs, :],
            lambda a: consensus[a : a + dirs],
            lambda a: own_ref[base + a : base + a + dirs, :],
            dirs,
        )
        for a in jones:
            jones_ref[a : a + dirs, chunk * width : (chunk + 1) * width] = jones[a]
        store_native(chunk, width, dirs, shared, shared_ref)


def native_kernel(rows_ref, out_ref):
    dirs = out_ref.shape[0]
    rows = {a: rows_ref[a : a + dirs, :] for a in range(0, 8 * dirs, dirs)}
    store_native(0, rows_ref.shape[1], dirs, rows, out_ref)


def partial_coeffs_kernel(weights_ref, *refs):
    units, out_ref = refs[:-1], refs[-1]
    weights = weights_ref[...]
    for k in range(out_ref.shape[1]):
        for part in range(2):
            for i in range(2):
                values = [ref[k, part, i] for ref in units]
                for m in range(weights.shape[0]):
                    out_ref[m, k, part, i] = weighted(weights, m, values)


def final_kernel(basis_ref, weights_ref, own_ref, partial_ref, *refs):
    units, (coeffs_hbm, dual_hbm, coeffs_ref, dual_ref, sems) = refs[:-5], refs[-5:]
    terms, dirs = coeffs_ref.shape[:2]
    weights = weights_ref[:, weights_ref.shape[1] - len(units) :]
    copies = []
    for k in range(dirs):
        for part in range(2):
            for i in range(2):
                values = [ref[k, part, i] for ref in units]
                consensus = None
                for m in range(terms):
                    total = partial_ref[m, k, part, i] + weighted(weights, m, values)
                    coeffs_ref[m, k, part, i] = total
                    share = total * jnp.broadcast_to(basis_ref[0:1, m : m + 1], total.shape)
                    consensus = share if consensus is None else consensus + share
                dual_ref[k, part, i] = RHO * (own_ref[k, part, i] - consensus)
        copies.append(pltpu.make_async_copy(coeffs_ref.at[:, k], coeffs_hbm.at[:, k], sems.at[k]))
        copies[-1].start()
    copies.append(pltpu.make_async_copy(dual_ref, dual_hbm, sems.at[dirs]))
    copies[-1].start()
    for copy in copies:
        copy.wait()


def struct(*shape, dtype=jnp.float32):
    return jax.ShapeDtypeStruct(shape, dtype)


def call(kernel, out_shape, first, args, scratch=(), space=VMEM, out_space=VMEM):
    many = isinstance(out_shape, (tuple, list))
    return pl.pallas_call(
        kernel,
        out_shape=out_shape,
        in_specs=[space if at else first for at in range(len(args))],
        out_specs=tuple(out_space for _ in out_shape) if many else out_space,
        scratch_shapes=list(scratch),
        compiler_params=PARAMS,
    )(*args)


def swap(value, axis, bit):
    size = lax.axis_size(axis)
    return lax.ppermute(value, axis, [(i, i ^ bit) for i in range(size)])


def sum_over_dir(mine, other):
    size = lax.axis_size("dir")
    mine = mine + swap(other, "dir", 1)
    bit = 2
    while bit < size:
        far = swap(mine, "dir", bit)
        mine = mine + far
        bit *= 2
    return mine, swap(mine, "dir", 1)


def gather_bands(value):
    half = lax.axis_size("band") // 2
    far = swap(value, "band", half)
    near = [value]
    for bit in range(1, half):
        near.append(swap(value, "band", bit))
    passed = [far]
    for bit in range(1, half):
        passed.append(swap(far, "band", bit))
    return near + passed


def reduce_bands(shared, row, factor):
    sums = lax.psum(row.reshape((-1,) + (1,) * shared.ndim) * shared[None], "band")
    flat = sums.reshape(sums.shape[0], -1)
    return jax.scipy.linalg.cho_solve((factor, True), flat).reshape(sums.shape)


def local(visibilities, coherencies, jones_start, dual_start, consensus_start, freq_basis, pairs):
    row = freq_basis[0]
    terms = row.shape[0]
    bands = lax.axis_size("band")
    vis, coher = visibilities[0], coherencies[0]
    native = jones_start.shape[1:]
    dirs, stations = native[0], native[-1]
    times, baselines = coher.shape[-2:]
    rows = 8 * dirs
    parity = jnp.broadcast_to((lax.axis_index("dir") % 2).astype(jnp.int32), (SUBLANES, LANES))
    chunked = stations % (bands * LANES) == 0 and bands > 2 and bands & (bands - 1) == 0
    hi = lax.Precision.HIGHEST
    width = stations // bands if chunked else LANES
    chunks = stations // width
    half = struct(2, 2, times, baselines)
    flat = struct(rows, stations)
    spread_rows = struct(chunks, rows, width)
    onehot = pltpu.VMEM((stations, 2 * baselines), jnp.bfloat16)
    left = pltpu.VMEM((12 * dirs, 2 * baselines), jnp.float32)
    model_out = (struct(rows, 2 * baselines), half, half)

    if not chunked:
        gram = lax.psum(row[:, None] * row[None, :], "band") + RIDGE * bands * jnp.eye(terms, dtype=jnp.float32)
        factor = jnp.linalg.cholesky(gram)

    def model(jones):
        return call(model_kernel, model_out, VMEM, (parity, jones, pairs, coher), [onehot])

    def station_sums(gathered, mine, other):
        base = call(
            normal_kernel, struct(chunks, 12 * dirs, width), VMEM, (gathered, pairs, coher),
            [onehot, pltpu.VMEM((4 * dirs, 2 * baselines), jnp.float32), left],
        )
        mine, other = sum_over_dir(mine, other)
        return call(
            right_kernel, struct(chunks, 12 * dirs, width), VMEM,
            (parity, gathered, pairs, coher, vis, mine, other, base),
            [onehot, pltpu.VMEM((rows, 2 * baselines), jnp.float32)],
        )

    def share(shared):
        coeffs = reduce_bands(shared, row, factor)
        return coeffs, jnp.tensordot(row, coeffs, axes=(0, 0), precision=hi)

    started = call(
        first_model_kernel, model_out, VMEM,
        (parity, *(pltpu.with_memory_space_constraint(x, pltpu.HBM) for x in (jones_start[0], pairs, coher))),
        [
            onehot,
            pltpu.VMEM((rows, stations), jnp.float32),
            pltpu.VMEM(native, jnp.float32),
            pltpu.VMEM(pairs.shape, pairs.dtype),
            pltpu.VMEM(coher.shape, jnp.float32),
            pltpu.SemaphoreType.DMA((3,)),
        ],
        HBM,
    )
    known, lag = call(prepare_kernel, (spread_rows,) * 2, SMEM, (freq_basis, dual_start[0], consensus_start))
    jones, unit = call(
        first_update_kernel, (flat, struct(stations * rows // width + SUBLANES, width)), VMEM,
        (freq_basis, station_sums(*started), known, lag),
    )
    if chunked:
        early = bands // 2 + 1
        units = gather_bands(unit)
        started = model(jones)
        sums = station_sums(*started)
        jones, unit, spread, basis = call(
            gathered_update_kernel,
            (flat, struct(chunks * rows, width), struct(1, bands), struct(bands, terms)), VMEM, (sums, *units),
        )
        units = gather_bands(unit)
        started = model(jones)
        sums = station_sums(*started)
        partial = call(partial_consensus_kernel, struct(chunks * rows, width), VMEM, (spread, *units[:early]))
        jones, shared = call(
            gathered_last_kernel, (flat, struct(*native)), VMEM, (spread, sums, unit, partial, *units[early:])
        )
        jones = call(native_kernel, struct(*native), VMEM, (jones,))
        units = gather_bands(shared)
        weights = call(weights_kernel, struct(terms, bands), VMEM, (basis,))
        partial = call(partial_coeffs_kernel, struct(terms, *native), VMEM, (weights, *units[:early]))
        coeffs, dual = call(
            final_kernel, (struct(terms, *native), struct(*native)), VMEM,
            (freq_basis, weights, shared, partial, *units[early:]),
            [
                pltpu.VMEM((terms, *native), jnp.float32),
                pltpu.VMEM(native, jnp.float32),
                pltpu.SemaphoreType.DMA((dirs + 1,)),
            ],
            out_space=HBM,
        )
    else:
        shared = unit[: chunks * rows].reshape(spread_rows.shape)
        for _ in range(ITERS - 2):
            consensus = share(shared)[1]
            sums = station_sums(*model(jones))
            jones, shared = call(update_kernel, (flat, spread_rows), VMEM, (sums, consensus, shared))
        consensus = share(shared)[1]
        sums = station_sums(*model(jones))
        jones, shared = call(last_update_kernel, (struct(*native),) * 2, VMEM, (sums, consensus, shared))
        coeffs, consensus = share(shared)
        dual = RHO * (shared - consensus)
    return jones[None], dual[None], coeffs


def solution(mesh):
    in_specs = (
        P("band", None, None, None, None, None),
        P("band", "dir", None, None, None, None, None),
        P("band", "dir", None, None, None, None),
        P("band", "dir", None, None, None, None),
        P(None, "dir", None, None, None, None),
        P("band", None),
        P(),
    )
    out_specs = (
        P("band", "dir", None, None, None, None),
        P("band", "dir", None, None, None, None),
        P(None, "dir", None, None, None, None),
    )

    return jax.shard_map(local, mesh=mesh, in_specs=in_specs, out_specs=out_specs, check_vma=False)
```
